8 devices in a mesh: rep: 1 (over z), dp: 8 (over x, y, core).
Axes of the slice: x: 2, y: 2, z: 1, core: 2. Of those that a mesh axis runs over, the one named last changes fastest.
Arguments:
- g_w_gate: bfloat16 [8, 2, 1024, 3072], P(('rep', 'dp'))
- g_w_up: bfloat16 [8, 2, 1024, 3072], P(('rep', 'dp'))
- g_w_down: bfloat16 [8, 2, 3072, 1024], P(('rep', 'dp'))
- w_gate: bfloat16 [2, 1024, 3072], replicated
- w_up: bfloat16 [2, 1024, 3072], replicated
- w_down: bfloat16 [2, 3072, 1024], replicated
- m_w_gate: float32 [2, 1024, 3072], P(None, 'dp')
- m_w_up: float32 [2, 1024, 3072], P(None, 'dp')
- m_w_down: float32 [2, 3072, 1024], P(None, 'dp')
- v_w_gate: float32 [2, 1024, 3072], P(None, 'dp')
- v_w_up: float32 [2, 1024, 3072], P(None, 'dp')
- v_w_down: float32 [2, 3072, 1024], P(None, 'dp')
Outputs:
- output 1: bfloat16 [2, 1024, 3072], P('rep')
- output 2: bfloat16 [2, 1024, 3072], P('rep')
- output 3: bfloat16 [2, 3072, 1024], P('rep')
- output 4: float32 [2, 1024, 3072], P('rep', 'dp')
- output 5: float32 [2, 1024, 3072], P('rep', 'dp')
- output 6: float32 [2, 3072, 1024], P('rep', 'dp')
- output 7: float32 [2, 1024, 3072], P('rep', 'dp')
- output 8: float32 [2, 1024, 3072], P('rep', 'dp')
- output 9: float32 [2, 3072, 1024], P('rep', 'dp')
All inputs are finite; a program needn't handle non-finite values.
Results may differ from the reference program's by a relative error of at most 0.022.
Values are sent between devices in bfloat16 or wider.
A program may use at most 2 GiB of HBM per device.

```python
import jax
import jax.numpy as jnp
from jax import lax

DEVICES = 8
D = 1024
FF = 3072
LAYERS = 2
NAMES = ("w_gate", "w_up", "w_down")
SHAPES = {"w_gate": (LAYERS, D, FF), "w_up": (LAYERS, D, FF), "w_down": (LAYERS, FF, D)}


def setup_inputs(seed: int = 0, part: int = 0) -> dict:
    kz, *keys = jax.random.split(jax.random.key(seed), 1 + 5 * len(NAMES))
    loud = 2.0 ** jax.random.uniform(kz, (), jnp.float32, -1.0, 1.0)
    drawn = {}
    for name, key, both in zip(NAMES, keys[:3], keys[3:6], strict=True):
        own = jax.random.normal(jax.random.fold_in(key, part), (DEVICES, *SHAPES[name]), jnp.float32)
        shared = jax.random.normal(jax.random.fold_in(both, part), SHAPES[name], jnp.float32)
        drawn["g_" + name] = (loud * (0.7 * shared / DEVICES + 0.7 * own * DEVICES**-0.5)).astype(jnp.bfloat16)
    for name, key in zip(NAMES, keys[6:9], strict=True):
        drawn[name] = (jax.random.normal(key, SHAPES[name], jnp.float32) * SHAPES[name][1] ** -0.5).astype(jnp.bfloat16)
    for name, key in zip(NAMES, keys[9:12], strict=True):
        drawn["m_" + name] = loud * 0.5 * jax.random.normal(key, SHAPES[name], jnp.float32)
    for name, key in zip(NAMES, keys[12:15], strict=True):
        drawn["v_" + name] = loud * loud * jax.random.uniform(key, SHAPES[name], jnp.float32, 0.5, 1.5)
    return drawn


def adamw(w, m, v, g):
    m = 0.9 * m + 0.1 * g
    v = 0.95 * v + 0.05 * g * g
    step = m * lax.rsqrt(v + 1e-8) + 0.1 * w
    return (w - 0.02 * step).astype(jnp.bfloat16), m, v


def reference(g_w_gate, g_w_up, g_w_down, w_gate, w_up, w_down, m_w_gate, m_w_up, m_w_down, v_w_gate, v_w_up, v_w_down):
    def total(terms):
        return lax.scan(lambda so_far, term: (so_far + term.astype(jnp.float32), None), jnp.zeros(terms.shape[1:], jnp.float32), terms)[0]

    gradients = [total(terms).astype(jnp.bfloat16).astype(jnp.float32) for terms in (g_w_gate, g_w_up, g_w_down)]
    new = [
        adamw(w.astype(jnp.float32), m, v, g)
        for w, m, v, g in zip((w_gate, w_up, w_down), (m_w_gate, m_w_up, m_w_down), (v_w_gate, v_w_up, v_w_down), gradients, strict=True)
    ]
    return tuple(one[which] for which in range(3) for one in new)
```

```python
import jax
import jax.numpy as jnp
from jax import lax
from jax.experimental import pallas as pl
from jax.experimental.pallas import tpu as pltpu
from jax.sharding import PartitionSpec as P

LAYERS = 2
SUBS = 4
CHUNKS = LAYERS * SUBS
RING = 4
ROWS = (128, 128, 384)
COLS = (3072, 3072, 1024)
TILE = (16, 256)
MESH = pl.DeviceIdType.MESH
BF16, F32 = jnp.bfloat16, jnp.float32


def tiles(rows, cols, body, tile=TILE):
    across = cols // tile[1]

    def one(i, carry):
        row, col = lax.div(i, across), lax.rem(i, across)
        body(pl.multiple_of(row * tile[0], tile[0]), pl.multiple_of(col * tile[1], tile[1]))
        return carry

    lax.fori_loop(0, (rows // tile[0]) * across, one, 0)


def kernel(*refs):
    refs = list(refs)

    def take(n):
        out, refs[:n] = refs[:n], []
        return out

    g, w, m, v = take(3), take(3), take(3), take(3)
    w_out, m_out, v_out = take(3), take(3), take(3)
    core, first, second, own = take(3), take(3), take(3), take(3)
    fresh, w_in, m_in, v_in, m_new, v_new = take(3), take(3), take(3), take(3), take(3), take(3)
    core_sem, own_sem, first_sem, second_sem, block_sem, diag_sem, in_sem, mv_sem, send_sem, gather_sem = take(10)

    me = lax.axis_index("dp")
    x, y, c = lax.div(me, 4), lax.rem(lax.div(me, 2), 2), lax.rem(me, 2)
    to_core = {"dp": me + 1 - 2 * c}
    to_x = {"dp": me + 4 - 8 * x}
    to_y = {"dp": me + 2 - 4 * y}

    barrier = pltpu.get_barrier_semaphore()
    for peer in (to_core, to_x, to_y):
        pl.semaphore_signal(barrier, inc=1, device_id=peer, device_id_type=MESH)
    pl.semaphore_wait(barrier, 3)

    def remote(src, dst, send, recv, peer):
        return pltpu.make_async_remote_copy(src_ref=src, dst_ref=dst, send_sem=send, recv_sem=recv, device_id=peer, device_id_type=MESH)

    def local(src, dst, sem):
        return pltpu.make_async_copy(src, dst, sem)

    def where(t):
        return lax.div(t, SUBS), lax.rem(t, SUBS)

    size = [r // SUBS for r in ROWS]
    half = [r // SUBS // 2 for r in ROWS]

    def core_copy(i, t):
        layer, sub = where(t)
        rows = pl.ds(pl.multiple_of(sub * size[i], size[i]), size[i])
        return remote(g[i].at[layer, :, :, 1 - c, rows, :], core[i].at[t], send_sem.at[0, i], core_sem.at[t, i], to_core)

    def own_copy(i, t):
        layer, sub = where(t)
        rows = pl.ds(pl.multiple_of(sub * size[i], size[i]), size[i])
        return local(g[i].at[layer, :, :, c, rows, :], own[i].at[lax.rem(t, RING)], own_sem.at[lax.rem(t, RING), i])

    def first_copy(i, t, axis):
        if axis == 0:
            src, peer = core[i].at[t, 1 - x, :, pl.ds(0, half[i]), :], to_x
        else:
            src, peer = core[i].at[t, :, 1 - y, pl.ds(half[i], half[i]), :], to_y
        return remote(src, first[i].at[t, axis], send_sem.at[1, i], first_sem.at[t, axis, i], peer)

    def second_copy(i, t, axis):
        if axis == 0:
            src, peer = core[i].at[t, x, 1 - y, pl.ds(0, half[i]), :], to_y
        else:
            src, peer = core[i].at[t, 1 - x, y, pl.ds(half[i], half[i]), :], to_x
        return remote(src, second[i].at[t, axis], send_sem.at[2, i], second_sem.at[t, axis, i], peer)

    def block(i, t, owner, part=None):
        layer, sub = where(t)
        start, n = owner * ROWS[i] + sub * size[i], size[i]
        if part is not None:
            start, n = start + part * half[i], half[i]
        return w_out[i].at[layer, pl.ds(pl.multiple_of(start, half[i]), n), :]

    by_x, by_y, across = me + 4 - 8 * x, me + 2 - 4 * y, me + 6 - 8 * x - 4 * y

    def block_copies(i, t):
        src, dst = fresh[i].at[t], block(i, t, me)
        return [
            remote(src, dst, send_sem.at[3, i], block_sem.at[t, 0, i], to_x),
            remote(src, dst, send_sem.at[3, i], block_sem.at[t, 1, i], to_y),
            remote(src, dst, send_sem.at[3, i], gather_sem.at[i], to_core),
            local(src, dst, send_sem.at[3, i]),
        ]

    def diag_copy(i, t, axis):
        owner, peer = (by_y, to_x) if axis == 0 else (by_x, to_y)
        ref = block(i, t, owner, axis)
        return remote(ref, ref, send_sem.at[4, i], diag_sem.at[t, axis, i], peer)

    def block_to_core(i, t, axis):
        ref = block(i, t, by_x if axis == 0 else by_y)
        return remote(ref, ref, send_sem.at[5, i], gather_sem.at[i], to_core)

    def diag_to_core(i, t, axis):
        ref = block(i, t, across, axis)
        return remote(ref, ref, send_sem.at[6, i], gather_sem.at[i], to_core)

    def in_copies(i, t):
        layer, sub = where(t)
        rows = pl.ds(pl.multiple_of(sub * size[i], size[i]), size[i])
        mine = pl.ds(pl.multiple_of(me * ROWS[i] + sub * size[i], size[i]), size[i])
        return [
            local(w[i].at[layer, mine, :], w_in[i], in_sem.at[0, i]),
            local(m[i].at[layer, rows, :], m_in[i], in_sem.at[1, i]),
            local(v[i].at[layer, rows, :], v_in[i], in_sem.at[2, i]),
        ]

    def mv_copies(i, t):
        layer, sub = where(t)
        rows = pl.ds(pl.multiple_of(sub * size[i], size[i]), size[i])
        return [
            local(m_new[i], m_out[i].at[layer, rows, :], mv_sem.at[0, i]),
            local(v_new[i], v_out[i].at[layer, rows, :], mv_sem.at[1, i]),
        ]

    def start_core(t):
        for i in range(3):
            core_copy(i, t).start()

    def start_own(t):
        for i in range(3):
            own_copy(i, t).start()

    def reduce_first(t):
        slot = lax.rem(t, RING)
        for i in range(3):
            core_copy(i, t).wait_recv()
            own_copy(i, t).wait()
            for a in range(2):
                for axis in range(2):
                    bx, by = (1 - x, a) if axis == 0 else (a, 1 - y)

                    def add(row, col, i=i, bx=bx, by=by, axis=axis):
                        at = (pl.ds(axis * half[i] + row, TILE[0]), pl.ds(col, TILE[1]))
                        mine = own[i][(slot, bx, by, *at)].astype(F32)
                        core[i][(t, bx, by, *at)] = (mine + core[i][(t, bx, by, *at)].astype(F32)).astype(BF16)

                    tiles(half[i], COLS[i], add)
            for axis in range(2):
                first_copy(i, t, axis).start()

    def reduce_second(t):
        slot = lax.rem(t, RING)
        for i in range(3):
            for axis in range(2):
                first_copy(i, t, axis).wait_recv()
                bx, by = (x, 1 - y) if axis == 0 else (1 - x, y)
                came = 1 - y if axis == 0 else 1 - x

                def add(row, col, i=i, bx=bx, by=by, axis=axis, came=came):
                    at = (pl.ds(axis * half[i] + row, TILE[0]), pl.ds(col, TILE[1]))
                    mine = own[i][(slot, bx, by, *at)].astype(F32) + core[i][(t, bx, by, *at)].astype(F32)
                    other = first[i][t, axis, came, pl.ds(row, TILE[0]), pl.ds(col, TILE[1])].astype(F32)
                    core[i][(t, bx, by, *at)] = (mine + other).astype(BF16)

                tiles(half[i], COLS[i], add)
                second_copy(i, t, axis).start()

    def update(t):
        slot = lax.rem(t, RING)
        for i in range(3):
            for copy in in_copies(i, t):
                copy.wait()

            @pl.when(t > 0)
            def _(i=i):
                for copy in mv_copies(i, t - 1):
                    copy.wait()

            for axis in range(2):
                second_copy(i, t, axis).wait_recv()
                came = y if axis == 0 else x

                def adamw(row, col, i=i, axis=axis, came=came):
                    at = (pl.ds(axis * half[i] + row, TILE[0]), pl.ds(col, TILE[1]))
                    there = (pl.ds(row, TILE[0]), pl.ds(col, TILE[1]))
                    total = own[i][(slot, x, y, *at)].astype(F32) + core[i][(t, x, y, *at)].astype(F32)
                    total = total + first[i][(t, axis, came, *there)].astype(F32) + second[i][(t, axis, *there)].astype(F32)
                    grad = total.astype(BF16).astype(F32)
                    weight = w_in[i][at].astype(F32)
                    mm = 0.9 * m_in[i][at] + 0.1 * grad
                    vv = 0.95 * v_in[i][at] + 0.05 * grad * grad
                    step = mm * lax.rsqrt(vv + 1e-8) + 0.1 * weight
                    m_new[i][at] = mm
                    v_new[i][at] = vv
                    fresh[i][(t, *at)] = (weight - 0.02 * step).astype(BF16)

                tiles(half[i], COLS[i], adamw)
            for copy in block_copies(i, t) + mv_copies(i, t):
                copy.start()

            @pl.when(t + 1 < CHUNKS)
            def _(i=i):
                for copy in in_copies(i, t + 1):
                    copy.start()

    def forward(t):
        for i in range(3):
            came = block_copies(i, t)
            came[1].wait_recv()
            diag_copy(i, t, 0).start()
            came[0].wait_recv()
            diag_copy(i, t, 1).start()
            for axis in range(2):
                block_to_core(i, t, axis).start()

    def finish(t):
        for i in range(3):
            for axis in range(2):
                diag_copy(i, t, axis).wait_recv()
                diag_to_core(i, t, axis).start()

    start_core(0)
    start_own(0)
    start_core(1)
    for i in range(3):
        for copy in in_copies(i, 0):
            copy.start()

    def step(k, carry):
        @pl.when(k < CHUNKS - 2)
        def _():
            start_core(k + 2)

        @pl.when(k < CHUNKS - 1)
        def _():
            start_own(k + 1)

        for lag, stage in enumerate((reduce_first, reduce_second, update, forward, finish)):

            @pl.when(jnp.logical_and(k >= lag, k < CHUNKS + lag))
            def _(lag=lag, stage=stage):
                stage(k - lag)

        return carry

    lax.fori_loop(0, CHUNKS + 4, step, 0)

    for i in range(3):
        for copy in mv_copies(i, CHUNKS - 1):
            copy.wait()
        part = w_out[i].at[:, pl.ds(0, 4 * ROWS[i]), :]
        local(part, part, gather_sem.at[i]).wait()
        for kind, ref in ((0, core[i]), (1, first[i]), (2, second[i]), (3, part), (4, fresh[i]), (5, first[i]), (6, fresh[i])):
            local(ref, ref, send_sem.at[kind, i]).wait()


def scratch(lead, dtype=BF16, lane=lambda i: ROWS[i] // SUBS):
    return [pltpu.VMEM((*lead, lane(i), COLS[i]), dtype) for i in range(3)]


def step(*arrays):
    g, w, m, v = (arrays[i : i + 3] for i in (0, 3, 6, 9))
    g = [t.reshape(LAYERS, 2, 2, 2, ROWS[i], COLS[i]) for i, t in enumerate(g)]
    halves = lambda i: ROWS[i] // SUBS // 2
    dma = pltpu.SemaphoreType.DMA
    out = pl.pallas_call(
        kernel,
        out_shape=[jax.ShapeDtypeStruct(t.shape, t.dtype) for t in (*w, *m, *v)],
        in_specs=[pl.BlockSpec(memory_space=pl.ANY)] * 12,
        out_specs=[pl.BlockSpec(memory_space=pl.ANY)] * 9,
        scratch_shapes=[
            *scratch((CHUNKS, 2, 2)),
            *scratch((CHUNKS, 2, 2), lane=halves),
            *scratch((CHUNKS, 2), lane=halves),
            *scratch((RING, 2, 2)),
            *scratch((CHUNKS,)),
            *scratch(()),
            *scratch((), F32),
            *scratch((), F32),
            *scratch((), F32),
            *scratch((), F32),
            dma((CHUNKS, 3)),
            dma((RING, 3)),
            dma((CHUNKS, 2, 3)),
            dma((CHUNKS, 2, 3)),
            dma((CHUNKS, 2, 3)),
            dma((CHUNKS, 2, 3)),
            dma((3, 3)),
            dma((2, 3)),
            dma((7, 3)),
            dma((3,)),
        ],
        compiler_params=pltpu.CompilerParams(collective_id=0, has_side_effects=True, vmem_limit_bytes=60 * 2**20),
        name="step",
    )(*g, *w, *m, *v)
    return tuple(out)


def solution(mesh):
    all_of, cut = P(None, None, None), P(None, "dp", None)
    return jax.shard_map(
        step,
        mesh=mesh,
        in_specs=(P(("rep", "dp"), None, None, None),) * 3 + (all_of,) * 3 + (cut,) * 6,
        out_specs=(P("rep", None, None),) * 3 + (P("rep", "dp", None),) * 6,
        check_vma=False,
    )
```

```python
import jax
import jax.numpy as jnp
from jax import lax
from jax.experimental import pallas as pl
from jax.experimental.pallas import tpu as pltpu
from jax.sharding import PartitionSpec as P

LAYERS = 2
SUBS = 4
CHUNKS = LAYERS * SUBS
RING = 4
EARLY = 3
LATE = CHUNKS - EARLY
ROWS = (128, 128, 384)
COLS = (3072, 3072, 1024)
TILE = (16, 256)
MESH = pl.DeviceIdType.MESH
BF16, F32 = jnp.bfloat16, jnp.float32


def tiles(rows, cols, body, tile=TILE):
    across = cols // tile[1]

    def one(i, carry):
        row, col = lax.div(i, across), lax.rem(i, across)
        body(pl.multiple_of(row * tile[0], tile[0]), pl.multiple_of(col * tile[1], tile[1]))
        return carry

    lax.fori_loop(0, (rows // tile[0]) * across, one, 0)


def kernel(*refs):
    refs = list(refs)

    def take(n):
        out, refs[:n] = refs[:n], []
        return out

    g, w, m, v = take(3), take(3), take(3), take(3)
    w_out, m_out, v_out, pass_on = take(3), take(3), take(3), take(2)
    core, first, second, own, held = take(3), take(3), take(3), take(3), take(3)
    fresh, w_in, m_in, v_in, m_new, v_new = take(3), take(3), take(3), take(3), take(3), take(3)
    core_sem, own_sem, first_sem, second_sem, block_sem, diag_sem, in_sem, mv_sem, send_sem, gather_sem, keep_sem = take(11)

    me = lax.axis_index("dp")
    x, y, c = lax.div(me, 4), lax.rem(lax.div(me, 2), 2), lax.rem(me, 2)
    to_core = {"dp": me + 1 - 2 * c}
    to_x = {"dp": me + 4 - 8 * x}
    to_y = {"dp": me + 2 - 4 * y}

    barrier = pltpu.get_barrier_semaphore()
    for peer in (to_core, to_x, to_y):
        pl.semaphore_signal(barrier, inc=1, device_id=peer, device_id_type=MESH)
    pl.semaphore_wait(barrier, 3)

    def remote(src, dst, send, recv, peer):
        return pltpu.make_async_remote_copy(src_ref=src, dst_ref=dst, send_sem=send, recv_sem=recv, device_id=peer, device_id_type=MESH)

    def local(src, dst, sem):
        return pltpu.make_async_copy(src, dst, sem)

    def where(t):
        return lax.div(t, SUBS), lax.rem(t, SUBS)

    size = [r // SUBS for r in ROWS]
    half = [r // SUBS // 2 for r in ROWS]

    def core_copy(i, t):
        layer, sub = where(t)
        rows = pl.ds(pl.multiple_of(sub * size[i], size[i]), size[i])
        return remote(g[i].at[layer, :, :, 1 - c, rows, :], core[i].at[t], send_sem.at[0, i], core_sem.at[t, i], to_core)

    def own_copy(i, t):
        layer, sub = where(t)
        rows = pl.ds(pl.multiple_of(sub * size[i], size[i]), size[i])
        return local(g[i].at[layer, :, :, c, rows, :], own[i].at[lax.rem(t, RING)], own_sem.at[lax.rem(t, RING), i])

    def first_copy(i, t, axis):
        if axis == 0:
            src, peer = core[i].at[t, 1 - x, :, pl.ds(0, half[i]), :], to_x
        else:
            src, peer = core[i].at[t, :, 1 - y, pl.ds(half[i], half[i]), :], to_y
        return remote(src, first[i].at[t, axis], send_sem.at[1, i], first_sem.at[t, axis, i], peer)

    def second_copy(i, t, axis):
        if axis == 0:
            src, peer = core[i].at[t, x, 1 - y, pl.ds(0, half[i]), :], to_y
        else:
            src, peer = core[i].at[t, 1 - x, y, pl.ds(half[i], half[i]), :], to_x
        return remote(src, second[i].at[t, axis], send_sem.at[2, i], second_sem.at[t, axis, i], peer)

    def block(i, t, owner, part=None):
        layer, sub = where(t)
        start, n = owner * ROWS[i] + sub * size[i], size[i]
        if part is not None:
            start, n = start + part * half[i], half[i]
        return w_out[i].at[layer, pl.ds(pl.multiple_of(start, half[i]), n), :]

    by_x, by_y, across = me + 4 - 8 * x, me + 2 - 4 * y, me + 6 - 8 * x - 4 * y

    def block_copies(i, t):
        src, dst = fresh[i].at[t], block(i, t, me)
        return [
            remote(src, dst, send_sem.at[3, i], gather_sem.at[0, i], to_core),
            local(src, dst, send_sem.at[3, i]),
        ]

    def block_copy(i, t, axis, late):
        src, dst = fresh[i].at[t], held[i].at[t - EARLY, axis] if late else block(i, t, me)
        return remote(src, dst, send_sem.at[3, i], block_sem.at[t, axis, i], to_y if axis else to_x)

    def keep_copies(i, t, axis):
        j = t - EARLY
        owner, part, src = (by_x, 1, held[i].at[j, 0]) if axis == 0 else (by_y, 0, held[i].at[j, 1])
        out = [local(src, block(i, t, owner), keep_sem.at[0, i])]
        dst = pass_on[part].at[i, j]
        for row, col, rows, cols in PIECES[i]:
            from_ = src.at[pl.ds(part * half[i] + row, rows), :]
            out.append(local(from_, dst.at[:, pl.ds(col, cols)], keep_sem.at[1, i]))
        return out

    def diag_copy(i, t, axis):
        owner, peer = (by_y, to_x) if axis == 0 else (by_x, to_y)
        ref = block(i, t, owner, axis)
        return remote(ref, ref, send_sem.at[4, i], diag_sem.at[t, axis, i], peer)

    def block_to_core(i, t, axis, late):
        ref = block(i, t, by_x if axis == 0 else by_y)
        src = held[i].at[t - EARLY, axis] if late else ref
        return remote(src, ref, send_sem.at[5, i], gather_sem.at[0, i], to_core)

    def diag_to_core(i, t, axis):
        ref = block(i, t, across, axis)
        return remote(ref, ref, send_sem.at[6, i], gather_sem.at[1, i], to_core)

    def in_copies(i, t):
        layer, sub = where(t)
        rows = pl.ds(pl.multiple_of(sub * size[i], size[i]), size[i])
        mine = pl.ds(pl.multiple_of(me * ROWS[i] + sub * size[i], size[i]), size[i])
        return [
            local(w[i].at[layer, mine, :], w_in[i], in_sem.at[0, i]),
            local(m[i].at[layer, rows, :], m_in[i], in_sem.at[1, i]),
            local(v[i].at[layer, rows, :], v_in[i], in_sem.at[2, i]),
        ]

    def mv_copies(i, t):
        layer, sub = where(t)
        rows = pl.ds(pl.multiple_of(sub * size[i], size[i]), size[i])
        return [
            local(m_new[i], m_out[i].at[layer, rows, :], mv_sem.at[0, i]),
            local(v_new[i], v_out[i].at[layer, rows, :], mv_sem.at[1, i]),
        ]

    def start_core(t):
        for i in range(3):
            core_copy(i, t).start()

    def start_own(t):
        for i in range(3):
            own_copy(i, t).start()

    def reduce_first(t):
        slot = lax.rem(t, RING)
        for i in range(3):
            core_copy(i, t).wait_recv()
            own_copy(i, t).wait()
            for a in range(2):
                for axis in range(2):
                    bx, by = (1 - x, a) if axis == 0 else (a, 1 - y)

                    def add(row, col, i=i, bx=bx, by=by, axis=axis):
                        at = (pl.ds(axis * half[i] + row, TILE[0]), pl.ds(col, TILE[1]))
                        mine = own[i][(slot, bx, by, *at)].astype(F32)
                        core[i][(t, bx, by, *at)] = (mine + core[i][(t, bx, by, *at)].astype(F32)).astype(BF16)

                    tiles(half[i], COLS[i], add)
            for axis in range(2):
                first_copy(i, t, axis).start()

    def reduce_second(t):
        slot = lax.rem(t, RING)
        for i in range(3):
            for axis in range(2):
                first_copy(i, t, axis).wait_recv()
                bx, by = (x, 1 - y) if axis == 0 else (1 - x, y)
                came = 1 - y if axis == 0 else 1 - x

                def add(row, col, i=i, bx=bx, by=by, axis=axis, came=came):
                    at = (pl.ds(axis * half[i] + row, TILE[0]), pl.ds(col, TILE[1]))
                    mine = own[i][(slot, bx, by, *at)].astype(F32) + core[i][(t, bx, by, *at)].astype(F32)
                    other = first[i][t, axis, came, pl.ds(row, TILE[0]), pl.ds(col, TILE[1])].astype(F32)
                    core[i][(t, bx, by, *at)] = (mine + other).astype(BF16)

                tiles(half[i], COLS[i], add)
                second_copy(i, t, axis).start()

    def update(t):
        slot = lax.rem(t, RING)
        for i in range(3):
            for copy in in_copies(i, t):
                copy.wait()

            @pl.when(t > 0)
            def _(i=i):
                for copy in mv_copies(i, t - 1):
                    copy.wait()

            for axis in range(2):
                second_copy(i, t, axis).wait_recv()
                came = y if axis == 0 else x

                def adamw(row, col, i=i, axis=axis, came=came):
                    at = (pl.ds(axis * half[i] + row, TILE[0]), pl.ds(col, TILE[1]))
                    there = (pl.ds(row, TILE[0]), pl.ds(col, TILE[1]))
                    total = own[i][(slot, x, y, *at)].astype(F32) + core[i][(t, x, y, *at)].astype(F32)
                    total = total + first[i][(t, axis, came, *there)].astype(F32) + second[i][(t, axis, *there)].astype(F32)
                    grad = total.astype(BF16).astype(F32)
                    weight = w_in[i][at].astype(F32)
                    mm = 0.9 * m_in[i][at] + 0.1 * grad
                    vv = 0.95 * v_in[i][at] + 0.05 * grad * grad
                    step = mm * lax.rsqrt(vv + 1e-8) + 0.1 * weight
                    m_new[i][at] = mm
                    v_new[i][at] = vv
                    fresh[i][(t, *at)] = (weight - 0.02 * step).astype(BF16)

                tiles(half[i], COLS[i], adamw)
            for late in (False, True):

                @pl.when(t >= EARLY if late else t < EARLY)
                def _(i=i, late=late):
                    for axis in range(2):
                        block_copy(i, t, axis, late).start()

            for copy in block_copies(i, t) + mv_copies(i, t):
                copy.start()

            @pl.when(t + 1 < CHUNKS)
            def _(i=i):
                for copy in in_copies(i, t + 1):
                    copy.start()

    def forward(t):
        @pl.when(t < EARLY)
        def _():
            for i in range(3):
                for axis in range(2):
                    block_copy(i, t, 1 - axis, False).wait_recv()
                    diag_copy(i, t, axis).start()
                for axis in range(2):
                    block_to_core(i, t, axis, False).start()

        @pl.when(t >= EARLY)
        def _():
            for i in range(3):
                for axis in range(2):
                    block_copy(i, t, axis, True).wait_recv()
                    block_to_core(i, t, axis, True).start()
                    for copy in keep_copies(i, t, axis):
                        copy.start()

    def finish(t):
        for i in range(3):
            for axis in range(2):
                diag_copy(i, t, axis).wait_recv()
                diag_to_core(i, t, axis).start()

    start_core(0)
    start_own(0)
    start_core(1)
    for i in range(3):
        for copy in in_copies(i, 0):
            copy.start()

    def step(k, carry):
        @pl.when(k < CHUNKS - 2)
        def _():
            start_core(k + 2)

        @pl.when(k < CHUNKS - 1)
        def _():
            start_own(k + 1)

        for lag, stage in enumerate((reduce_first, reduce_second, update, forward)):

            @pl.when(jnp.logical_and(k >= lag, k < CHUNKS + lag))
            def _(lag=lag, stage=stage):
                stage(k - lag)

        @pl.when(jnp.logical_and(k >= 4, k < EARLY + 4))
        def _():
            finish(k - 4)

        return carry

    lax.fori_loop(0, CHUNKS + 3, step, 0)

    for i in range(3):
        for copy in mv_copies(i, CHUNKS - 1):
            copy.wait()
        layers = w_out[i].at[:, pl.ds(0, 3 * ROWS[i]), :]
        early = fresh[i].at[pl.ds(0, EARLY)]
        local(layers, layers, gather_sem.at[0, i]).wait()
        local(early, early, gather_sem.at[1, i]).wait()
        part = w_out[i].at[:, pl.ds(0, 4 * ROWS[i]), :]
        for kind, ref in ((0, core[i]), (1, first[i]), (2, second[i]), (3, part), (4, early), (5, first[i]), (6, early)):
            local(ref, ref, send_sem.at[kind, i]).wait()
        local(held[i], held[i], keep_sem.at[0, i]).wait()
        late = fresh[i].at[pl.ds(0, LATE)]
        local(late, late, keep_sem.at[1, i]).wait()


PIECES = (((0, 0, 16, 3072),), ((0, 0, 16, 3072),), tuple((16 * p, 1024 * p, 16, 1024) for p in range(3)))


def write_out(*refs):
    refs = list(refs)

    def take(n):
        out, refs[:n] = refs[:n], []
        return out

    (me_ref,), w, mv, w_out, mv_out = take(1), take(3), take(6), take(3), take(6)
    ring, whole, (w_sem, mv_sem) = take(3), take(6), take(2)
    me = me_ref[0]
    x, y = lax.div(me, 4), lax.rem(lax.div(me, 2), 2)
    size = [r // SUBS for r in ROWS]
    jobs = 3 * CHUNKS + EARLY

    def copies(i, k):
        diag = k >= 3 * CHUNKS
        t = jnp.where(diag, k - 3 * CHUNKS, lax.div(k, 3))
        r = lax.rem(k, 3)
        bx = jnp.where(jnp.logical_or(diag, r == 1), 1 - x, x)
        by = jnp.where(jnp.logical_or(diag, r == 2), 1 - y, y)
        rows = pl.ds(pl.multiple_of(lax.rem(t, SUBS) * size[i], size[i]), size[i])
        at = (lax.div(t, SUBS), bx, by, slice(None), rows, slice(None))
        slot = lax.rem(k, DEEP)
        buf = ring[i].at[slot]
        return pltpu.make_async_copy(w[i].at[at], buf, w_sem.at[0, slot, i]), pltpu.make_async_copy(buf, w_out[i].at[at], w_sem.at[1, slot, i])

    ahead = DEEP // 2
    for i in range(6):
        pltpu.make_async_copy(mv[i], whole[i], mv_sem.at[0, i]).start()
    for k in range(ahead):
        for i in range(3):
            copies(i, jnp.int32(k))[0].start()
    for i in range(6):
        pltpu.make_async_copy(mv[i], whole[i], mv_sem.at[0, i]).wait()
        pltpu.make_async_copy(whole[i], mv_out[i], mv_sem.at[1, i]).start()

    def step(k, carry):
        for i in range(3):
            into, out = copies(i, k)
            into.wait()
            out.start()

            @pl.when(k >= ahead)
            def _(i=i):
                copies(i, k - ahead)[1].wait()

            @pl.when(k + ahead < jobs)
            def _(i=i):
                copies(i, k + ahead)[0].start()

        return carry

    lax.fori_loop(0, jobs, step, 0)
    for k in range(jobs - ahead, jobs):
        for i in range(3):
            copies(i, jnp.int32(k))[1].wait()
    for i in range(6):
        pltpu.make_async_copy(whole[i], mv_out[i], mv_sem.at[1, i]).wait()


DEEP = 8


def write_diag(me_ref, mine_a, mine_b, other_a, other_b, *refs):
    w_out, sem = refs[3:6], refs[6]
    me = me_ref[0]
    x, y, c = lax.div(me, 4), lax.rem(lax.div(me, 2), 2), lax.rem(me, 2)

    def each(j, carry):
        t = j + EARLY
        for i in range(3):
            size = ROWS[i] // SUBS
            for part, owner, src in ((0, c, mine_a), (1, c, mine_b), (0, 1 - c, other_a), (1, 1 - c, other_b)):
                start = (6 - 4 * x - 2 * y + owner) * ROWS[i] + lax.rem(t, SUBS) * size + part * (size // 2)
                for row, col, rows, cols in PIECES[i]:
                    dst = w_out[i].at[lax.div(t, SUBS), pl.ds(pl.multiple_of(start + row, 16), rows), :]
                    pltpu.make_async_copy(src.at[i, j, :, pl.ds(col, cols)], dst, sem).start()
        return carry

    lax.fori_loop(0, LATE, each, 0)
    for src in (mine_a, mine_b, other_a, other_b):
        pltpu.make_async_copy(src, src, sem).wait()


def scratch(lead, dtype=BF16, lane=lambda i: ROWS[i] // SUBS):
    return [pltpu.VMEM((*lead, lane(i), COLS[i]), dtype) for i in range(3)]


def step(*arrays):
    g, w, m, v = (arrays[i : i + 3] for i in (0, 3, 6, 9))
    g = [t.reshape(LAYERS, 2, 2, 2, ROWS[i], COLS[i]) for i, t in enumerate(g)]
    halves = lambda i: ROWS[i] // SUBS // 2
    dma = pltpu.SemaphoreType.DMA
    hbm = pl.BlockSpec(memory_space=pltpu.HBM)
    like = [jax.ShapeDtypeStruct(t.shape, t.dtype) for t in (*w, *m, *v)]
    out = pl.pallas_call(
        kernel,
        out_shape=like + [jax.ShapeDtypeStruct((3, LATE, 16, 3072), BF16)] * 2,
        in_specs=[hbm] * 12,
        out_specs=[hbm] * 11,
        scratch_shapes=[
            *scratch((CHUNKS, 2, 2)),
            *scratch((CHUNKS, 2, 2), lane=halves),
            *scratch((CHUNKS, 2), lane=halves),
            *scratch((RING, 2, 2)),
            *scratch((LATE, 2)),
            *scratch((CHUNKS,)),
            *scratch(()),
            *scratch((), F32),
            *scratch((), F32),
            *scratch((), F32),
            *scratch((), F32),
            dma((CHUNKS, 3)),
            dma((RING, 3)),
            dma((CHUNKS, 2, 3)),
            dma((CHUNKS, 2, 3)),
            dma((CHUNKS, 2, 3)),
            dma((CHUNKS, 2, 3)),
            dma((3, 3)),
            dma((2, 3)),
            dma((7, 3)),
            dma((2, 3)),
            dma((2, 3)),
        ],
        compiler_params=pltpu.CompilerParams(collective_id=0, has_side_effects=True, vmem_limit_bytes=62 * 2**20),
        name="step",
    )(*g, *w, *m, *v)
    gathered, moments, pass_on = out[:3], out[3:9], out[9:]

    def swap(t, far):
        return lax.ppermute(t, "dp", [(i, i ^ far) for i in range(8)])

    with jax.named_scope("late"):
        mine = [swap(pass_on[0], 4), swap(pass_on[1], 2)]

    me = lax.axis_index("dp").astype(jnp.int32).reshape(1)
    smem = pl.BlockSpec(memory_space=pltpu.SMEM)
    blocks = [t.reshape(LAYERS, 2, 2, 2, ROWS[i], COLS[i]) for i, t in enumerate(gathered)]
    written = pl.pallas_call(
        write_out,
        out_shape=[jax.ShapeDtypeStruct(t.shape, t.dtype) for t in (*blocks, *moments)],
        in_specs=[smem] + [hbm] * 9,
        out_specs=[hbm] * 9,
        scratch_shapes=[
            *(pltpu.VMEM((DEEP, 2, ROWS[i] // SUBS, COLS[i]), BF16) for i in range(3)),
            *(pltpu.VMEM(t.shape, F32) for t in moments),
            dma((2, DEEP, 3)),
            dma((2, 6)),
        ],
        compiler_params=pltpu.CompilerParams(vmem_limit_bytes=60 * 2**20),
        cost_estimate=pl.CostEstimate(flops=2_000_000_000, bytes_accessed=100_000_000, transcendentals=0),
        name="write_out",
    )(me, *blocks, *moments)
    mine, written = lax.optimization_barrier((mine, written))

    with jax.named_scope("exchange"):
        other = [swap(t, 1) for t in mine]
    whole = [t.reshape(w[i].shape) for i, t in enumerate(written[:3])]
    vmem = pl.BlockSpec(memory_space=pltpu.VMEM)
    whole = pl.pallas_call(
        write_diag,
        out_shape=like[:3],
        in_specs=[smem] + [vmem] * 4 + [hbm] * 3,
        out_specs=[hbm] * 3,
        scratch_shapes=[dma],
        input_output_aliases={5: 0, 6: 1, 7: 2},
        compiler_params=pltpu.CompilerParams(vmem_limit_bytes=8 * 2**20),
        name="write_diag",
    )(me, *mine, *other, *whole)
    return (*whole, *written[3:])


def solution(mesh):
    all_of, cut = P(None, None, None), P(None, "dp", None)
    return jax.shard_map(
        step,
        mesh=mesh,
        in_specs=(P(("rep", "dp"), None, None, None),) * 3 + (all_of,) * 3 + (cut,) * 6,
        out_specs=(P("rep", None, None),) * 3 + (P("rep", "dp", None),) * 6,
        check_vma=False,
    )
```

```python
import functools

import jax
import jax.numpy as jnp
from jax import lax
from jax.experimental import pallas as pl
from jax.experimental.pallas import tpu as pltpu
from jax.sharding import PartitionSpec as P


LAYERS = 2
SUBS = 4
CHUNKS = LAYERS * SUBS
RING = 4
EARLY = 2
GROUPS = (4, 2)
LATE = CHUNKS - EARLY
ROWS = (128, 128, 384)
COLS = (3072, 3072, 1024)
TILE = (16, 256)
WIDE = (16, 512)
MESH = pl.DeviceIdType.MESH
BF16, F32 = jnp.bfloat16, jnp.float32


def tiles(rows, cols, body, tile=TILE):
    across = cols // tile[1]

    def one(i, carry):
        row, col = lax.div(i, across), lax.rem(i, across)
        body(pl.multiple_of(row * tile[0], tile[0]), pl.multiple_of(col * tile[1], tile[1]))
        return carry

    lax.fori_loop(0, (rows // tile[0]) * across, one, 0)


def kernel(*refs):
    refs = list(refs)

    def take(n):
        out, refs[:n] = refs[:n], []
        return out

    g, w, m, v = take(3), take(3), take(3), take(3)
    w_out, m_out, v_out, pass_on = take(3), take(3), take(3), (take(2), take(2))
    core, first, second, own, held = take(3), take(3), take(3), take(3), take(3)
    fresh, w_in, m_in, v_in, m_new, v_new = take(3), take(3), take(3), take(3), take(3), take(3)
    core_sem, own_sem, first_sem, second_sem, block_sem, diag_sem, in_sem, mv_sem, send_sem, gather_sem, keep_sem = take(11)

    me = lax.axis_index("dp")
    x, y, c = lax.div(me, 4), lax.rem(lax.div(me, 2), 2), lax.rem(me, 2)
    to_core = {"dp": me + 1 - 2 * c}
    to_x = {"dp": me + 4 - 8 * x}
    to_y = {"dp": me + 2 - 4 * y}

    barrier = pltpu.get_barrier_semaphore()
    for peer in (to_core, to_x, to_y):
        pl.semaphore_signal(barrier, inc=1, device_id=peer, device_id_type=MESH)
    pl.semaphore_wait(barrier, 3)

    def remote(src, dst, send, recv, peer):
        return pltpu.make_async_remote_copy(src_ref=src, dst_ref=dst, send_sem=send, recv_sem=recv, device_id=peer, device_id_type=MESH)

    def local(src, dst, sem):
        return pltpu.make_async_copy(src, dst, sem)

    def where(t):
        return lax.div(t, SUBS), lax.rem(t, SUBS)

    size = [r // SUBS for r in ROWS]
    half = [r // SUBS // 2 for r in ROWS]

    def core_copy(i, t):
        layer, sub = where(t)
        rows = pl.ds(pl.multiple_of(sub * size[i], size[i]), size[i])
        return remote(g[i].at[layer, :, :, 1 - c, rows, :], core[i].at[t], send_sem.at[0, i], core_sem.at[t, i], to_core)

    def own_copy(i, t):
        layer, sub = where(t)
        rows = pl.ds(pl.multiple_of(sub * size[i], size[i]), size[i])
        return local(g[i].at[layer, :, :, c, rows, :], own[i].at[lax.rem(t, RING)], own_sem.at[lax.rem(t, RING), i])

    def first_copy(i, t, axis):
        if axis == 0:
            src, peer = core[i].at[t, 1 - x, :, pl.ds(0, half[i]), :], to_x
        else:
            src, peer = core[i].at[t, :, 1 - y, pl.ds(half[i], half[i]), :], to_y
        return remote(src, first[i].at[t, axis], send_sem.at[1, i], first_sem.at[t, axis, i], peer)

    def second_copy(i, t, axis):
        if axis == 0:
            src, peer = core[i].at[t, x, 1 - y, pl.ds(0, half[i]), :], to_y
        else:
            src, peer = core[i].at[t, 1 - x, y, pl.ds(half[i], half[i]), :], to_x
        return remote(src, second[i].at[t, axis], send_sem.at[2, i], second_sem.at[t, axis, i], peer)

    def block(i, t, owner, part=None):
        layer, sub = where(t)
        start, n = owner * ROWS[i] + sub * size[i], size[i]
        if part is not None:
            start, n = start + part * half[i], half[i]
        return w_out[i].at[layer, pl.ds(pl.multiple_of(start, half[i]), n), :]

    by_x, by_y, across = me + 4 - 8 * x, me + 2 - 4 * y, me + 6 - 8 * x - 4 * y

    def block_copies(i, t):
        src, dst = fresh[i].at[t], block(i, t, me)
        return [
            remote(src, dst, send_sem.at[3, i], gather_sem.at[0, i], to_core),
            local(src, dst, send_sem.at[3, i]),
        ]

    def block_copy(i, t, axis, late):
        src, dst = fresh[i].at[t], held[i].at[t - EARLY, axis] if late else block(i, t, me)
        return remote(src, dst, send_sem.at[3, i], block_sem.at[t, axis, i], to_y if axis else to_x)

    def keep_copies(i, t, axis, group):
        j = t - EARLY
        owner, part, src = (by_x, 1, held[i].at[j, 0]) if axis == 0 else (by_y, 0, held[i].at[j, 1])
        out = [local(src, block(i, t, owner), keep_sem.at[0, i])]
        dst = pass_on[group][part].at[i, j - sum(GROUPS[:group])]
        for row, col, rows, cols in PIECES[i]:
            from_ = src.at[pl.ds(part * half[i] + row, rows), :]
            out.append(local(from_, dst.at[:, pl.ds(col, cols)], keep_sem.at[1, i]))
        return out

    def diag_copy(i, t, axis):
        owner, peer = (by_y, to_x) if axis == 0 else (by_x, to_y)
        ref = block(i, t, owner, axis)
        return remote(ref, ref, send_sem.at[4, i], diag_sem.at[t, axis, i], peer)

    def block_to_core(i, t, axis, late):
        ref = block(i, t, by_x if axis == 0 else by_y)
        src = held[i].at[t - EARLY, axis] if late else ref
        return remote(src, ref, send_sem.at[5, i], gather_sem.at[0, i], to_core)

    def diag_to_core(i, t, axis):
        ref = block(i, t, across, axis)
        return remote(ref, ref, send_sem.at[6, i], gather_sem.at[1, i], to_core)

    def in_copies(i, t):
        layer, sub = where(t)
        rows = pl.ds(pl.multiple_of(sub * size[i], size[i]), size[i])
        mine = pl.ds(pl.multiple_of(me * ROWS[i] + sub * size[i], size[i]), size[i])
        return [
            local(w[i].at[layer, mine, :], w_in[i], in_sem.at[0, i]),
            local(m[i].at[layer, rows, :], m_in[i], in_sem.at[1, i]),
            local(v[i].at[layer, rows, :], v_in[i], in_sem.at[2, i]),
        ]

    def mv_copies(i, t):
        layer, sub = where(t)
        rows = pl.ds(pl.multiple_of(sub * size[i], size[i]), size[i])
        return [
            local(m_new[i], m_out[i].at[layer, rows, :], mv_sem.at[0, i]),
            local(v_new[i], v_out[i].at[layer, rows, :], mv_sem.at[1, i]),
        ]

    def start_core(t):
        for i in range(3):
            core_copy(i, t).start()

    def start_own(t):
        for i in range(3):
            own_copy(i, t).start()

    def reduce_first(t):
        slot = lax.rem(t, RING)
        for i in range(3):
            core_copy(i, t).wait_recv()
            own_copy(i, t).wait()
            for axis in range(2):
                for a in range(2):
                    bx, by = (1 - x, a) if axis == 0 else (a, 1 - y)

                    def add(row, col, i=i, bx=bx, by=by, axis=axis):
                        at = (pl.ds(axis * half[i] + row, WIDE[0]), pl.ds(col, WIDE[1]))
                        mine = own[i][(slot, bx, by, *at)].astype(F32)
                        core[i][(t, bx, by, *at)] = (mine + core[i][(t, bx, by, *at)].astype(F32)).astype(BF16)

                    tiles(half[i], COLS[i], add, WIDE)
                first_copy(i, t, axis).start()

    def reduce_second(t):
        slot = lax.rem(t, RING)
        for i in range(3):
            for axis in range(2):
                first_copy(i, t, axis).wait_recv()
                bx, by = (x, 1 - y) if axis == 0 else (1 - x, y)
                came = 1 - y if axis == 0 else 1 - x

                def add(row, col, i=i, bx=bx, by=by, axis=axis, came=came):
                    at = (pl.ds(axis * half[i] + row, WIDE[0]), pl.ds(col, WIDE[1]))
                    mine = own[i][(slot, bx, by, *at)].astype(F32) + core[i][(t, bx, by, *at)].astype(F32)
                    other = first[i][t, axis, came, pl.ds(row, WIDE[0]), pl.ds(col, WIDE[1])].astype(F32)
                    core[i][(t, bx, by, *at)] = (mine + other).astype(BF16)

                tiles(half[i], COLS[i], add, WIDE)
                second_copy(i, t, axis).start()

    def update(t):
        slot = lax.rem(t, RING)
        for i in range(3):
            for copy in in_copies(i, t):
                copy.wait()

            @pl.when(t > 0)
            def _(i=i):
                for copy in mv_copies(i, t - 1):
                    copy.wait()

            for axis in range(2):
                second_copy(i, t, axis).wait_recv()
                came = y if axis == 0 else x

                def adamw(row, col, i=i, axis=axis, came=came):
                    at = (pl.ds(axis * half[i] + row, TILE[0]), pl.ds(col, TILE[1]))
                    there = (pl.ds(row, TILE[0]), pl.ds(col, TILE[1]))
                    total = own[i][(slot, x, y, *at)].astype(F32) + core[i][(t, x, y, *at)].astype(F32)
                    total = total + first[i][(t, axis, came, *there)].astype(F32) + second[i][(t, axis, *there)].astype(F32)
                    grad = total.astype(BF16).astype(F32)
                    weight = w_in[i][at].astype(F32)
                    mm = 0.9 * m_in[i][at] + 0.1 * grad
                    vv = 0.95 * v_in[i][at] + 0.05 * grad * grad
                    step = mm * lax.rsqrt(vv + 1e-8) + 0.1 * weight
                    m_new[i][at] = mm
                    v_new[i][at] = vv
                    fresh[i][(t, *at)] = (weight - 0.02 * step).astype(BF16)

                tiles(half[i], COLS[i], adamw)
            for late in (False, True):

                @pl.when(t >= EARLY if late else t < EARLY)
                def _(i=i, late=late):
                    for axis in range(2):
                        block_copy(i, t, axis, late).start()

            for copy in block_copies(i, t) + mv_copies(i, t):
                copy.start()

            @pl.when(t + 1 < CHUNKS)
            def _(i=i):
                for copy in in_copies(i, t + 1):
                    copy.start()

    def forward(t):
        @pl.when(t < EARLY)
        def _():
            for i in range(3):
                for axis in range(2):
                    block_copy(i, t, 1 - axis, False).wait_recv()
                    diag_copy(i, t, axis).start()
                for axis in range(2):
                    block_to_core(i, t, axis, False).start()

        for group in range(2):
            start = EARLY + sum(GROUPS[:group])

            @pl.when(jnp.logical_and(t >= start, t < start + GROUPS[group]))
            def _(group=group):
                for i in range(3):
                    for axis in range(2):
                        block_copy(i, t, axis, True).wait_recv()
                        for copy in keep_copies(i, t, axis, group):
                            copy.start()
                        block_to_core(i, t, axis, True).start()

    def finish(t):
        for i in range(3):
            for axis in range(2):
                diag_copy(i, t, axis).wait_recv()
                diag_to_core(i, t, axis).start()

    start_core(0)
    start_own(0)
    start_core(1)
    for i in range(3):
        for copy in in_copies(i, 0):
            copy.start()

    def step(k, carry):
        @pl.when(k < CHUNKS - 2)
        def _():
            start_core(k + 2)

        @pl.when(k < CHUNKS - 1)
        def _():
            start_own(k + 1)

        for lag, stage in enumerate((reduce_first, reduce_second, update, forward)):

            @pl.when(jnp.logical_and(k >= lag, k < CHUNKS + lag))
            def _(lag=lag, stage=stage):
                stage(k - lag)

        @pl.when(jnp.logical_and(k >= 4, k < EARLY + 4))
        def _():
            finish(k - 4)

        return carry

    lax.fori_loop(0, CHUNKS + 3, step, 0)

    for i in range(3):
        for copy in mv_copies(i, CHUNKS - 1):
            copy.wait()
        layers = w_out[i].at[:, pl.ds(0, 3 * ROWS[i]), :]
        early = fresh[i].at[pl.ds(0, EARLY)]
        local(layers, layers, gather_sem.at[0, i]).wait()
        local(early, early, gather_sem.at[1, i]).wait()
        part = w_out[i].at[:, pl.ds(0, 4 * ROWS[i]), :]
        for kind, ref in ((0, core[i]), (1, first[i]), (2, second[i]), (3, part), (4, early), (5, first[i]), (6, early)):
            local(ref, ref, send_sem.at[kind, i]).wait()
        local(held[i], held[i], keep_sem.at[0, i]).wait()
        late = fresh[i].at[pl.ds(0, LATE)]
        local(late, late, keep_sem.at[1, i]).wait()


PIECES = (((0, 0, 16, 3072),), ((0, 0, 16, 3072),), tuple((16 * p, 1024 * p, 16, 1024) for p in range(3)))


def write_weights(me_ref, *refs):
    w, w_out, ring, sem = refs[:3], refs[3:6], refs[6:9], refs[9]
    me = me_ref[0]
    x, y = lax.div(me, 4), lax.rem(lax.div(me, 2), 2)
    size = [r // SUBS for r in ROWS]
    jobs = 3 * CHUNKS + EARLY

    def copies(i, k):
        diag = k >= 3 * CHUNKS
        t = jnp.where(diag, k - 3 * CHUNKS, lax.div(k, 3))
        r = lax.rem(k, 3)
        bx = jnp.where(jnp.logical_or(diag, r == 1), 1 - x, x)
        by = jnp.where(jnp.logical_or(diag, r == 2), 1 - y, y)
        rows = pl.ds(pl.multiple_of(lax.rem(t, SUBS) * size[i], size[i]), size[i])
        at = (lax.div(t, SUBS), bx, by, slice(None), rows, slice(None))
        slot = lax.rem(k, DEEP)
        buf = ring[i].at[slot]
        return pltpu.make_async_copy(w[i].at[at], buf, sem.at[0, slot, i]), pltpu.make_async_copy(buf, w_out[i].at[at], sem.at[1, slot, i])

    ahead = DEEP // 2
    for k in range(ahead):
        for i in range(3):
            copies(i, jnp.int32(k))[0].start()

    def step(k, carry):
        for i in range(3):
            into, out = copies(i, k)
            into.wait()
            out.start()

            @pl.when(k >= ahead)
            def _(i=i):
                copies(i, k - ahead)[1].wait()

            @pl.when(k + ahead < jobs)
            def _(i=i):
                copies(i, k + ahead)[0].start()

        return carry

    lax.fori_loop(0, jobs, step, 0)
    for k in range(jobs - ahead, jobs):
        for i in range(3):
            copies(i, jnp.int32(k))[1].wait()


DEEP = 16


def write_moments(*refs):
    src, dst, buf, sem = refs[:6], refs[6:12], refs[12:18], refs[18]

    def copies(i, n):
        at = (n // 4, pl.ds(n % 4 * (src[i].shape[1] // 4), src[i].shape[1] // 4))
        return pltpu.make_async_copy(src[i].at[at], buf[i].at[at], sem.at[0, i, n]), pltpu.make_async_copy(buf[i].at[at], dst[i].at[at], sem.at[1, i, n])

    every = [(i, n) for i in range(6) for n in range(8)]
    for job in every:
        copies(*job)[0].start()
    for job in every:
        copies(*job)[0].wait()
        copies(*job)[1].start()
    for job in every:
        copies(*job)[1].wait()


def write_diag(start, me_ref, mine_a, mine_b, other_a, other_b, *refs):
    w_out, sem = refs[3:6], refs[6]
    me = me_ref[0]
    x, y, c = lax.div(me, 4), lax.rem(lax.div(me, 2), 2), lax.rem(me, 2)

    def each(j, carry):
        t = j + start
        for i in range(3):
            size = ROWS[i] // SUBS
            for part, owner, src in ((0, c, mine_a), (1, c, mine_b), (0, 1 - c, other_a), (1, 1 - c, other_b)):
                first = (6 - 4 * x - 2 * y + owner) * ROWS[i] + lax.rem(t, SUBS) * size + part * (size // 2)
                for row, col, rows, cols in PIECES[i]:
                    dst = w_out[i].at[lax.div(t, SUBS), pl.ds(pl.multiple_of(first + row, 16), rows), :]
                    pltpu.make_async_copy(src.at[i, j, :, pl.ds(col, cols)], dst, sem).start()
        return carry

    lax.fori_loop(0, mine_a.shape[1], each, 0)
    for src in (mine_a, mine_b, other_a, other_b):
        pltpu.make_async_copy(src, src, sem).wait()


def scratch(lead, dtype=BF16, lane=lambda i: ROWS[i] // SUBS):
    return [pltpu.VMEM((*lead, lane(i), COLS[i]), dtype) for i in range(3)]


def step(*arrays):
    g, w, m, v = (arrays[i : i + 3] for i in (0, 3, 6, 9))
    g = [t.reshape(LAYERS, 2, 2, 2, ROWS[i], COLS[i]) for i, t in enumerate(g)]
    halves = lambda i: ROWS[i] // SUBS // 2
    dma = pltpu.SemaphoreType.DMA
    hbm = pl.BlockSpec(memory_space=pltpu.HBM)
    like = [jax.ShapeDtypeStruct(t.shape, t.dtype) for t in (*w, *m, *v)]
    out = pl.pallas_call(
        kernel,
        out_shape=like + [jax.ShapeDtypeStruct((3, n, 16, 3072), BF16) for n in GROUPS for _ in range(2)],
        in_specs=[hbm] * 12,
        out_specs=[hbm] * 13,
        scratch_shapes=[
            *scratch((CHUNKS, 2, 2)),
            *scratch((CHUNKS, 2, 2), lane=halves),
            *scratch((CHUNKS, 2), lane=halves),
            *scratch((RING, 2, 2)),
            *scratch((LATE, 2)),
            *scratch((CHUNKS,)),
            *scratch(()),
            *scratch((), F32),
            *scratch((), F32),
            *scratch((), F32),
            *scratch((), F32),
            dma((CHUNKS, 3)),
            dma((RING, 3)),
            dma((CHUNKS, 2, 3)),
            dma((CHUNKS, 2, 3)),
            dma((CHUNKS, 2, 3)),
            dma((CHUNKS, 2, 3)),
            dma((3, 3)),
            dma((2, 3)),
            dma((7, 3)),
            dma((2, 3)),
            dma((2, 3)),
        ],
        compiler_params=pltpu.CompilerParams(collective_id=0, has_side_effects=True, vmem_limit_bytes=62 * 2**20),
        name="step",
    )(*g, *w, *m, *v)
    gathered, moments, pass_on = out[:3], out[3:9], (out[9:11], out[11:])

    def swap(t, far):
        return lax.ppermute(t, "dp", [(i, i ^ far) for i in range(8)])

    mine = []
    for group, pair in enumerate(pass_on):
        mine.append([])
        for part, far in ((0, 4), (1, 2)):
            mine[group].append(swap(pair[part], far))

    me = lax.axis_index("dp").astype(jnp.int32).reshape(1)
    smem, vmem = pl.BlockSpec(memory_space=pltpu.SMEM), pl.BlockSpec(memory_space=pltpu.VMEM)
    blocks = [t.reshape(LAYERS, 2, 2, 2, ROWS[i], COLS[i]) for i, t in enumerate(gathered)]
    weights = pl.pallas_call(
        write_weights,
        out_shape=[jax.ShapeDtypeStruct(t.shape, t.dtype) for t in blocks],
        in_specs=[smem] + [hbm] * 3,
        out_specs=[hbm] * 3,
        scratch_shapes=[*(pltpu.VMEM((DEEP, 2, ROWS[i] // SUBS, COLS[i]), BF16) for i in range(3)), dma((2, DEEP, 3))],
        compiler_params=pltpu.CompilerParams(vmem_limit_bytes=59 * 2**20),
        cost_estimate=pl.CostEstimate(flops=2_000_000_000, bytes_accessed=60_000_000, transcendentals=0),
        name="write_weights",
    )
    whole = weights(me, *blocks)
    mine[0], whole, moments = lax.optimization_barrier((mine[0], whole, moments))
    other = [[swap(t, 1) for t in mine[0]]]
    moments = pl.pallas_call(
        write_moments,
        out_shape=like[3:],
        in_specs=[hbm] * 6,
        out_specs=[hbm] * 6,
        scratch_shapes=[*(pltpu.VMEM(t.shape, F32) for t in moments), dma((2, 6, 8))],
        compiler_params=pltpu.CompilerParams(vmem_limit_bytes=57 * 2**20),
        cost_estimate=pl.CostEstimate(flops=2_000_000_000, bytes_accessed=36_000_000, transcendentals=0),
        name="write_moments",
    )(*moments)
    mine[1], moments = lax.optimization_barrier((mine[1], moments))
    other.append([swap(t, 1) for t in mine[1]])
    whole = [t.reshape(w[i].shape) for i, t in enumerate(whole)]
    for group in range(2):
        whole = pl.pallas_call(
            functools.partial(write_diag, EARLY + sum(GROUPS[:group])),
            out_shape=like[:3],
            in_specs=[smem] + [vmem] * 4 + [hbm] * 3,
            out_specs=[hbm] * 3,
            scratch_shapes=[dma],
            input_output_aliases={5: 0, 6: 1, 7: 2},
            compiler_params=pltpu.CompilerParams(vmem_limit_bytes=8 * 2**20),
            cost_estimate=pl.CostEstimate(flops=100_000_000, bytes_accessed=6_000_000, transcendentals=0),
            name="write_diag",
        )(me, *mine[group], *other[group], *whole)
    return (*whole, *moments)


def solution(mesh):
    all_of, cut = P(None, None, None), P(None, "dp", None)
    return jax.shard_map(
        step,
        mesh=mesh,
        in_specs=(P(("rep", "dp"), None, None, None),) * 3 + (all_of,) * 3 + (cut,) * 6,
        out_specs=(P("rep", None, None),) * 3 + (P("rep", "dp", None),) * 6,
        check_vma=False,
    )
```

```python
import functools

import jax
import jax.numpy as jnp
from jax import lax
from jax.experimental import pallas as pl
from jax.experimental.pallas import tpu as pltpu
from jax.sharding import PartitionSpec as P


LAYERS = 2
SUBS = 4
CHUNKS = LAYERS * SUBS
RING = 4
GROUPS = (3, 3, 1, 1)
STARTS = tuple(sum(GROUPS[:group]) for group in range(len(GROUPS)))
LAST = CHUNKS - 1
ROWS = (128, 128, 384)
COLS = (3072, 3072, 1024)
TILE = (16, 256)
WIDE = (16, 512)
MESH = pl.DeviceIdType.MESH
BF16, F32 = jnp.bfloat16, jnp.float32


def tiles(rows, cols, body, tile=TILE):
    across = cols // tile[1]

    def one(i, carry):
        row, col = lax.div(i, across), lax.rem(i, across)
        body(pl.multiple_of(row * tile[0], tile[0]), pl.multiple_of(col * tile[1], tile[1]))
        return carry

    lax.fori_loop(0, (rows // tile[0]) * across, one, 0)


def kernel(*refs):
    refs = list(refs)

    def take(n):
        out, refs[:n] = refs[:n], []
        return out

    g, w, m, v = take(3), take(3), take(3), take(3)
    w_out, m_out, v_out = take(3), take(3), take(3)
    pass_on, (last,) = [take(2) for _ in GROUPS], take(1)
    core, first, second, own, held = take(3), take(3), take(3), take(3), take(3)
    fresh, w_in, m_in, v_in, m_new, v_new = take(3), take(3), take(3), take(3), take(3), take(3)
    core_sem, own_sem, first_sem, second_sem, block_sem, in_sem, mv_sem, send_sem, gather_sem, keep_sem = take(10)

    me = lax.axis_index("dp")
    x, y, c = lax.div(me, 4), lax.rem(lax.div(me, 2), 2), lax.rem(me, 2)
    to_core = {"dp": me + 1 - 2 * c}
    to_x = {"dp": me + 4 - 8 * x}
    to_y = {"dp": me + 2 - 4 * y}

    barrier = pltpu.get_barrier_semaphore()
    for peer in (to_core, to_x, to_y):
        pl.semaphore_signal(barrier, inc=1, device_id=peer, device_id_type=MESH)
    pl.semaphore_wait(barrier, 3)

    def remote(src, dst, send, recv, peer):
        return pltpu.make_async_remote_copy(src_ref=src, dst_ref=dst, send_sem=send, recv_sem=recv, device_id=peer, device_id_type=MESH)

    def local(src, dst, sem):
        return pltpu.make_async_copy(src, dst, sem)

    def where(t):
        return lax.div(t, SUBS), lax.rem(t, SUBS)

    size = [r // SUBS for r in ROWS]
    half = [r // SUBS // 2 for r in ROWS]

    def core_copy(i, t, piece):
        layer, sub = where(t)
        part = piece % 2
        lines = pl.ds(pl.multiple_of(sub * size[i] + part * half[i], half[i]), half[i])
        if part == 0:
            bx, by = 1 - x if piece == 0 else x, slice(None)
        else:
            bx, by = slice(None), 1 - y if piece == 1 else y
        dst = core[i].at[t, bx, by, pl.ds(part * half[i], half[i]), :]
        return remote(g[i].at[layer, bx, by, 1 - c, lines, :], dst, send_sem.at[0, i], core_sem.at[t, piece, i], to_core)

    def own_copy(i, t):
        layer, sub = where(t)
        rows = pl.ds(pl.multiple_of(sub * size[i], size[i]), size[i])
        return local(g[i].at[layer, :, :, c, rows, :], own[i].at[lax.rem(t, RING)], own_sem.at[lax.rem(t, RING), i])

    def first_copy(i, t, axis):
        if axis == 0:
            src, peer = core[i].at[t, 1 - x, :, pl.ds(0, half[i]), :], to_x
        else:
            src, peer = core[i].at[t, :, 1 - y, pl.ds(half[i], half[i]), :], to_y
        return remote(src, first[i].at[t, axis], send_sem.at[1, i], first_sem.at[t, axis, i], peer)

    def second_copy(i, t, axis):
        if axis == 0:
            src, peer = core[i].at[t, x, 1 - y, pl.ds(0, half[i]), :], to_y
        else:
            src, peer = core[i].at[t, 1 - x, y, pl.ds(half[i], half[i]), :], to_x
        return remote(src, second[i].at[t, axis], send_sem.at[2, i], second_sem.at[t, axis, i], peer)

    def block(i, t, owner):
        layer, sub = where(t)
        return w_out[i].at[layer, pl.ds(pl.multiple_of(owner * ROWS[i] + sub * size[i], size[i]), size[i]), :]

    by_x, by_y = me + 4 - 8 * x, me + 2 - 4 * y

    def block_copies(i, t):
        src, dst = fresh[i].at[t], block(i, t, me)
        return [
            remote(src, held[i].at[t, 0], send_sem.at[3, i], block_sem.at[t, 0, i], to_x),
            remote(src, held[i].at[t, 1], send_sem.at[3, i], block_sem.at[t, 1, i], to_y),
            remote(src, dst, send_sem.at[3, i], gather_sem.at[0, i], to_core),
            local(src, dst, send_sem.at[3, i]),
        ]

    def keep_copies(i, t, axis, group):
        owner, part = (by_x, 1) if axis == 0 else (by_y, 0)
        src, dst = held[i].at[t, axis], pass_on[group][part].at[i, t - STARTS[group]]
        out = [local(src, block(i, t, owner), keep_sem.at[0, i])]
        for row, col, rows, cols in PIECES[i]:
            out.append(local(src.at[pl.ds(part * half[i] + row, rows), :], dst.at[:, pl.ds(col, cols)], keep_sem.at[1, i]))
        return out

    def last_copies(i, axis):
        src, dst = held[i].at[LAST, axis], last.at[i, axis]
        return [
            local(src.at[pl.ds(part * half[i] + row, rows), :], dst.at[part, :, pl.ds(col, cols)], keep_sem.at[2, i])
            for part in range(2)
            for row, col, rows, cols in PIECES[i]
        ]

    def block_to_core(i, t, axis):
        dst = block(i, t, by_x if axis == 0 else by_y)
        return remote(held[i].at[t, axis], dst, send_sem.at[4, i], gather_sem.at[1, i], to_core)

    def in_copies(i, t):
        layer, sub = where(t)
        rows = pl.ds(pl.multiple_of(sub * size[i], size[i]), size[i])
        mine = pl.ds(pl.multiple_of(me * ROWS[i] + sub * size[i], size[i]), size[i])
        return [
            local(w[i].at[layer, mine, :], w_in[i], in_sem.at[0, i]),
            local(m[i].at[layer, rows, :], m_in[i], in_sem.at[1, i]),
            local(v[i].at[layer, rows, :], v_in[i], in_sem.at[2, i]),
        ]

    def mv_copies(i, t):
        layer, sub = where(t)
        rows = pl.ds(pl.multiple_of(sub * size[i], size[i]), size[i])
        return [
            local(m_new[i], m_out[i].at[layer, rows, :], mv_sem.at[0, i]),
            local(v_new[i], v_out[i].at[layer, rows, :], mv_sem.at[1, i]),
        ]

    def start_core(t, order=((0, 1), (2, 3))):
        for pieces in order:
            for i in range(3):
                for piece in pieces:
                    core_copy(i, t, piece).start()

    def start_own(t):
        for i in range(3):
            own_copy(i, t).start()

    def reduce_first(t):
        slot = lax.rem(t, RING)
        for i in range(3):
            own_copy(i, t).wait()
            for axis in range(2):
                core_copy(i, t, axis).wait_recv()
                for a in range(2):
                    bx, by = (1 - x, a) if axis == 0 else (a, 1 - y)

                    def add(row, col, i=i, bx=bx, by=by, axis=axis):
                        at = (pl.ds(axis * half[i] + row, WIDE[0]), pl.ds(col, WIDE[1]))
                        mine = own[i][(slot, bx, by, *at)].astype(F32)
                        core[i][(t, bx, by, *at)] = (mine + core[i][(t, bx, by, *at)].astype(F32)).astype(BF16)

                    tiles(half[i], COLS[i], add, WIDE)
                first_copy(i, t, axis).start()

    def reduce_second(t):
        slot = lax.rem(t, RING)
        for i in range(3):
            for axis in range(2):
                core_copy(i, t, axis + 2).wait_recv()
                first_copy(i, t, axis).wait_recv()
                bx, by = (x, 1 - y) if axis == 0 else (1 - x, y)
                came = 1 - y if axis == 0 else 1 - x

                def add(row, col, i=i, bx=bx, by=by, axis=axis, came=came):
                    at = (pl.ds(axis * half[i] + row, WIDE[0]), pl.ds(col, WIDE[1]))
                    mine = own[i][(slot, bx, by, *at)].astype(F32) + core[i][(t, bx, by, *at)].astype(F32)
                    other = first[i][t, axis, came, pl.ds(row, WIDE[0]), pl.ds(col, WIDE[1])].astype(F32)
                    core[i][(t, bx, by, *at)] = (mine + other).astype(BF16)

                tiles(half[i], COLS[i], add, WIDE)
                second_copy(i, t, axis).start()

    def update(t):
        slot = lax.rem(t, RING)
        for i in range(3):
            for copy in in_copies(i, t):
                copy.wait()

            @pl.when(t > 0)
            def _(i=i):
                for copy in mv_copies(i, t - 1):
                    copy.wait()

            for axis in range(2):
                second_copy(i, t, axis).wait_recv()
                came = y if axis == 0 else x

                def adamw(row, col, i=i, axis=axis, came=came):
                    at = (pl.ds(axis * half[i] + row, TILE[0]), pl.ds(col, TILE[1]))
                    there = (pl.ds(row, TILE[0]), pl.ds(col, TILE[1]))
                    total = own[i][(slot, x, y, *at)].astype(F32) + core[i][(t, x, y, *at)].astype(F32)
                    total = total + first[i][(t, axis, came, *there)].astype(F32) + second[i][(t, axis, *there)].astype(F32)
                    grad = total.astype(BF16).astype(F32)
                    weight = w_in[i][at].astype(F32)
                    mm = 0.9 * m_in[i][at] + 0.1 * grad
                    vv = 0.95 * v_in[i][at] + 0.05 * grad * grad
                    step = mm * lax.rsqrt(vv + 1e-8) + 0.1 * weight
                    m_new[i][at] = mm
                    v_new[i][at] = vv
                    fresh[i][(t, *at)] = (weight - 0.02 * step).astype(BF16)

                tiles(half[i], COLS[i], adamw)
            for copy in block_copies(i, t) + mv_copies(i, t):
                copy.start()

            @pl.when(t + 1 < CHUNKS)
            def _(i=i):
                for copy in in_copies(i, t + 1):
                    copy.start()

    def forward(t):
        for group, start in enumerate(STARTS):

            @pl.when(jnp.logical_and(t >= start, t < start + GROUPS[group]))
            def _(group=group):
                for i in range(3):
                    for axis in range(2):
                        block_copies(i, t)[axis].wait_recv()
                        for copy in keep_copies(i, t, axis, group):
                            copy.start()

                        @pl.when(t < LAST)
                        def _(i=i, axis=axis):
                            block_to_core(i, t, axis).start()

                        @pl.when(t == LAST)
                        def _(i=i, axis=axis):
                            for copy in last_copies(i, axis):
                                copy.start()

    @pl.when(c == 0)
    def _():
        start_core(0)
        start_core(1)

    @pl.when(c == 1)
    def _():
        start_core(1)
        start_core(0, ((2, 3), (0, 1)))

    start_own(0)
    for i in range(3):
        for copy in in_copies(i, 0):
            copy.start()

    def step(k, carry):
        @pl.when(k < CHUNKS - 2)
        def _():
            start_core(k + 2)

        @pl.when(k < CHUNKS - 1)
        def _():
            start_own(k + 1)

        for lag, stage in enumerate((reduce_first, reduce_second, update, forward)):

            @pl.when(jnp.logical_and(k >= lag, k < CHUNKS + lag))
            def _(lag=lag, stage=stage):
                stage(k - lag)

        return carry

    lax.fori_loop(0, CHUNKS + 3, step, 0)

    for i in range(3):
        for copy in mv_copies(i, LAST):
            copy.wait()
        part = w_out[i].at[:, pl.ds(0, 4 * ROWS[i]), :]
        most = held[i].at[pl.ds(0, LAST)]
        local(fresh[i], fresh[i], gather_sem.at[0, i]).wait()
        local(most, most, gather_sem.at[1, i]).wait()
        for kind, ref in ((0, core[i]), (1, first[i]), (2, second[i]), (3, part), (4, most)):
            local(ref, ref, send_sem.at[kind, i]).wait()
        for kind, ref in ((0, held[i]), (1, fresh[i]), (2, held[i].at[0])):
            local(ref, ref, keep_sem.at[kind, i]).wait()


PIECES = (((0, 0, 16, 3072),), ((0, 0, 16, 3072),), tuple((16 * p, 1024 * p, 16, 1024) for p in range(3)))


def write_weights(me_ref, *refs):
    w, w_out, ring, sem = refs[:3], refs[3:6], refs[6:9], refs[9]
    me = me_ref[0]
    x, y = lax.div(me, 4), lax.rem(lax.div(me, 2), 2)
    size = [r // SUBS for r in ROWS]
    jobs = 3 * CHUNKS

    def copies(i, k):
        t, r = lax.div(k, 3), lax.rem(k, 3)
        bx = jnp.where(r == 1, 1 - x, x)
        by = jnp.where(r == 2, 1 - y, y)
        rows = pl.ds(pl.multiple_of(lax.rem(t, SUBS) * size[i], size[i]), size[i])
        at = (lax.div(t, SUBS), bx, by, slice(None), rows, slice(None))
        slot = lax.rem(k, DEEP)
        buf = ring[i].at[slot]
        return pltpu.make_async_copy(w[i].at[at], buf, sem.at[0, slot, i]), pltpu.make_async_copy(buf, w_out[i].at[at], sem.at[1, slot, i])

    ahead = DEEP // 2
    for k in range(ahead):
        for i in range(3):
            copies(i, jnp.int32(k))[0].start()

    def step(k, carry):
        for i in range(3):
            into, out = copies(i, k)
            into.wait()
            out.start()

            @pl.when(k >= ahead)
            def _(i=i):
                copies(i, k - ahead)[1].wait()

            @pl.when(k + ahead < jobs)
            def _(i=i):
                copies(i, k + ahead)[0].start()

        return carry

    lax.fori_loop(0, jobs, step, 0)
    for k in range(jobs - ahead, jobs):
        for i in range(3):
            copies(i, jnp.int32(k))[1].wait()


DEEP = 16


def write_moments(*refs):
    src, dst, buf, sem = refs[:6], refs[6:12], refs[12:18], refs[18]

    def copies(i, n):
        at = (n // 4, pl.ds(n % 4 * (src[i].shape[1] // 4), src[i].shape[1] // 4))
        return pltpu.make_async_copy(src[i].at[at], buf[i].at[at], sem.at[0, i, n]), pltpu.make_async_copy(buf[i].at[at], dst[i].at[at], sem.at[1, i, n])

    every = [(i, n) for i in range(6) for n in range(8)]
    for job in every:
        copies(*job)[0].start()
    for job in every:
        copies(*job)[0].wait()
        copies(*job)[1].start()
    for job in every:
        copies(*job)[1].wait()


def write_diag(group, me_ref, mine_a, mine_b, other_a, other_b, *refs):
    if group == 0:
        last, refs = refs[0], refs[1:]
    w_out, sem = refs[3:6], refs[6]
    me = me_ref[0]
    x, y, c = lax.div(me, 4), lax.rem(lax.div(me, 2), 2), lax.rem(me, 2)

    def write(i, t, part, owner, src):
        size = ROWS[i] // SUBS
        start = owner * ROWS[i] + lax.rem(t, SUBS) * size + part * (size // 2)
        for row, col, rows, cols in PIECES[i]:
            dst = w_out[i].at[lax.div(t, SUBS), pl.ds(pl.multiple_of(start + row, 16), rows), :]
            pltpu.make_async_copy(src.at[:, pl.ds(col, cols)], dst, sem).start()

    def each(j, carry):
        diag = 6 - 4 * x - 2 * y
        for i in range(3):
            for part, owner, src in ((0, c, mine_a), (1, c, mine_b), (0, 1 - c, other_a), (1, 1 - c, other_b)):
                write(i, j + STARTS[group], part, diag + owner, src.at[i, j])
        return carry

    lax.fori_loop(0, GROUPS[group], each, 0)
    arrays = [mine_a, mine_b, other_a, other_b]
    if group == 0:
        arrays.append(last)
        for i in range(3):
            for axis, owner in ((0, 4 * (1 - x) + 2 * y + 1 - c), (1, 4 * x + 2 * (1 - y) + 1 - c)):
                for part in range(2):
                    write(i, jnp.int32(LAST), part, owner, last.at[i, axis, part])
    for src in arrays:
        pltpu.make_async_copy(src, src, sem).wait()


def scratch(lead, dtype=BF16, lane=lambda i: ROWS[i] // SUBS):
    return [pltpu.VMEM((*lead, lane(i), COLS[i]), dtype) for i in range(3)]


def step(*arrays):
    g, w, m, v = (arrays[i : i + 3] for i in (0, 3, 6, 9))
    g = [t.reshape(LAYERS, 2, 2, 2, ROWS[i], COLS[i]) for i, t in enumerate(g)]
    halves = lambda i: ROWS[i] // SUBS // 2
    dma = pltpu.SemaphoreType.DMA
    hbm = pl.BlockSpec(memory_space=pltpu.HBM)
    like = [jax.ShapeDtypeStruct(t.shape, t.dtype) for t in (*w, *m, *v)]
    out = pl.pallas_call(
        kernel,
        out_shape=like + [jax.ShapeDtypeStruct((3, n, 16, 3072), BF16) for n in GROUPS for _ in range(2)] + [jax.ShapeDtypeStruct((3, 2, 2, 16, 3072), BF16)],
        in_specs=[hbm] * 12,
        out_specs=[hbm] * (10 + 2 * len(GROUPS)),
        scratch_shapes=[
            *scratch((CHUNKS, 2, 2)),
            *scratch((CHUNKS, 2, 2), lane=halves),
            *scratch((CHUNKS, 2), lane=halves),
            *scratch((RING, 2, 2)),
            *scratch((CHUNKS, 2)),
            *scratch((CHUNKS,)),
            *scratch(()),
            *scratch((), F32),
            *scratch((), F32),
            *scratch((), F32),
            *scratch((), F32),
            dma((CHUNKS, 4, 3)),
            dma((RING, 3)),
            dma((CHUNKS, 2, 3)),
            dma((CHUNKS, 2, 3)),
            dma((CHUNKS, 2, 3)),
            dma((3, 3)),
            dma((2, 3)),
            dma((5, 3)),
            dma((2, 3)),
            dma((3, 3)),
        ],
        compiler_params=pltpu.CompilerParams(collective_id=0, has_side_effects=True, vmem_limit_bytes=62 * 2**20),
        name="step",
    )(*g, *w, *m, *v)
    gathered, moments, pass_on, last = out[:3], out[3:9], [out[9 + 2 * n : 11 + 2 * n] for n in range(len(GROUPS))], out[-1]

    def swap(t, far):
        return lax.ppermute(t, "dp", [(i, i ^ far) for i in range(8)])

    mine = [[swap(pair[0], 4), swap(pair[1], 2)] for pair in pass_on]
    other = [[swap(t, 1) for t in pair] for pair in mine]
    last = swap(last, 1)

    me = lax.axis_index("dp").astype(jnp.int32).reshape(1)
    smem, vmem = pl.BlockSpec(memory_space=pltpu.SMEM), pl.BlockSpec(memory_space=pltpu.VMEM)

    def writer(body, operands, in_specs, outs, scratch_shapes, limit, flops, aliases={}):
        return pl.pallas_call(
            body,
            out_shape=outs,
            in_specs=in_specs,
            out_specs=[hbm] * len(outs),
            scratch_shapes=scratch_shapes,
            input_output_aliases=aliases,
            compiler_params=pltpu.CompilerParams(vmem_limit_bytes=limit * 2**20),
            cost_estimate=pl.CostEstimate(flops=flops, bytes_accessed=flops // 40, transcendentals=0),
        )(*operands)

    blocks = [t.reshape(LAYERS, 2, 2, 2, ROWS[i], COLS[i]) for i, t in enumerate(gathered)]
    shapes = [jax.ShapeDtypeStruct(t.shape, t.dtype) for t in blocks]
    ring = [*(pltpu.VMEM((DEEP, 2, ROWS[i] // SUBS, COLS[i]), BF16) for i in range(3)), dma((2, DEEP, 3))]
    whole = writer(write_weights, (me, *blocks), [smem] + [hbm] * 3, shapes, ring, 57, 2_000_000_000)
    buffers = [*(pltpu.VMEM(t.shape, F32) for t in moments), dma((2, 6, 8))]
    moments = writer(write_moments, moments, [hbm] * 6, like[3:], buffers, 55, 1_400_000_000)
    whole = [t.reshape(w[i].shape) for i, t in enumerate(whole)]
    for n in range(len(GROUPS)):
        operands = (me, *mine[n], *other[n], *((last,) if n == 0 else ()), *whole)
        at = len(operands) - 3
        specs = [smem] + [vmem] * (at - 1) + [hbm] * 3
        body = functools.partial(write_diag, n)
        whole = writer(body, operands, specs, like[:3], [dma], 12, 100_000_000, {at + i: i for i in range(3)})
    return (*whole, *moments)


def solution(mesh):
    all_of, cut = P(None, None, None), P(None, "dp", None)
    return jax.shard_map(
        step,
        mesh=mesh,
        in_specs=(P(("rep", "dp"), None, None, None),) * 3 + (all_of,) * 3 + (cut,) * 6,
        out_specs=(P("rep", None, None),) * 3 + (P("rep", "dp", None),) * 6,
        check_vma=False,
    )
```

```python
import functools

import jax
import jax.numpy as jnp
from jax import lax
from jax.experimental import pallas as pl
from jax.experimental.pallas import tpu as pltpu
from jax.sharding import PartitionSpec as P


LAYERS = 2
SUBS = 4
CHUNKS = LAYERS * SUBS
RING = 4
GROUPS = (3, 3, 1, 1)
STARTS = tuple(sum(GROUPS[:group]) for group in range(len(GROUPS)))
LAST = CHUNKS - 1
WRITES = ((0,), (1,), (2,), (3,))
ROWS = (128, 128, 384)
COLS = (3072, 3072, 1024)
TILE = (16, 256)
WIDE = (16, 512)
MESH = pl.DeviceIdType.MESH
BF16, F32 = jnp.bfloat16, jnp.float32


def tiles(rows, cols, body, tile=TILE):
    across = cols // tile[1]

    def one(i, carry):
        row, col = lax.div(i, across), lax.rem(i, across)
        body(pl.multiple_of(row * tile[0], tile[0]), pl.multiple_of(col * tile[1], tile[1]))
        return carry

    lax.fori_loop(0, (rows // tile[0]) * across, one, 0)


def kernel(*refs):
    refs = list(refs)

    def take(n):
        out, refs[:n] = refs[:n], []
        return out

    g, w, m, v = take(3), take(3), take(3), take(3)
    w_out, m_out, v_out = take(3), take(3), take(3)
    pass_on, (last,) = [take(2) for _ in GROUPS], take(1)
    core, first, second, own, held = take(3), take(3), take(3), take(3), take(3)
    fresh, w_in, m_in, v_in, m_new, v_new = take(3), take(3), take(3), take(3), take(3), take(3)
    core_sem, own_sem, first_sem, second_sem, block_sem, in_sem, mv_sem, send_sem, gather_sem, keep_sem = take(10)

    me = lax.axis_index("dp")
    x, y, c = lax.div(me, 4), lax.rem(lax.div(me, 2), 2), lax.rem(me, 2)
    to_core = {"dp": me + 1 - 2 * c}
    to_x = {"dp": me + 4 - 8 * x}
    to_y = {"dp": me + 2 - 4 * y}

    barrier = pltpu.get_barrier_semaphore()
    for peer in (to_core, to_x, to_y):
        pl.semaphore_signal(barrier, inc=1, device_id=peer, device_id_type=MESH)
    pl.semaphore_wait(barrier, 3)

    def remote(src, dst, send, recv, peer):
        return pltpu.make_async_remote_copy(src_ref=src, dst_ref=dst, send_sem=send, recv_sem=recv, device_id=peer, device_id_type=MESH)

    def local(src, dst, sem):
        return pltpu.make_async_copy(src, dst, sem)

    def where(t):
        return lax.div(t, SUBS), lax.rem(t, SUBS)

    size = [r // SUBS for r in ROWS]
    half = [r // SUBS // 2 for r in ROWS]

    def core_copy(i, t, piece):
        layer, sub = where(t)
        part = piece % 2
        lines = pl.ds(pl.multiple_of(sub * size[i] + part * half[i], half[i]), half[i])
        if part == 0:
            bx, by = 1 - x if piece == 0 else x, slice(None)
        else:
            bx, by = slice(None), 1 - y if piece == 1 else y
        dst = core[i].at[t, bx, by, pl.ds(part * half[i], half[i]), :]
        return remote(g[i].at[layer, bx, by, 1 - c, lines, :], dst, send_sem.at[0, i], core_sem.at[t, piece, i], to_core)

    def own_copy(i, t):
        layer, sub = where(t)
        rows = pl.ds(pl.multiple_of(sub * size[i], size[i]), size[i])
        return local(g[i].at[layer, :, :, c, rows, :], own[i].at[lax.rem(t, RING)], own_sem.at[lax.rem(t, RING), i])

    def first_copy(i, t, axis):
        if axis == 0:
            src, peer = core[i].at[t, 1 - x, :, pl.ds(0, half[i]), :], to_x
        else:
            src, peer = core[i].at[t, :, 1 - y, pl.ds(half[i], half[i]), :], to_y
        return remote(src, first[i].at[t, axis], send_sem.at[1, i], first_sem.at[t, axis, i], peer)

    def second_copy(i, t, axis):
        if axis == 0:
            src, peer = core[i].at[t, x, 1 - y, pl.ds(0, half[i]), :], to_y
        else:
            src, peer = core[i].at[t, 1 - x, y, pl.ds(half[i], half[i]), :], to_x
        return remote(src, second[i].at[t, axis], send_sem.at[2, i], second_sem.at[t, axis, i], peer)

    def block(i, t, owner):
        layer, sub = where(t)
        return w_out[i].at[layer, pl.ds(pl.multiple_of(owner * ROWS[i] + sub * size[i], size[i]), size[i]), :]

    by_x, by_y = me + 4 - 8 * x, me + 2 - 4 * y

    def block_copies(i, t):
        src, dst = fresh[i].at[t], block(i, t, me)
        return [
            remote(src, held[i].at[t, 0], send_sem.at[3, i], block_sem.at[t, 0, i], to_x),
            remote(src, held[i].at[t, 1], send_sem.at[3, i], block_sem.at[t, 1, i], to_y),
            remote(src, dst, send_sem.at[3, i], gather_sem.at[0, i], to_core),
            local(src, dst, send_sem.at[3, i]),
        ]

    def keep_copies(i, t, axis, group):
        owner, part = (by_x, 1) if axis == 0 else (by_y, 0)
        src, dst = held[i].at[t, axis], pass_on[group][part].at[i, t - STARTS[group]]
        out = [local(src, block(i, t, owner), keep_sem.at[0, i])]
        for row, col, rows, cols in PIECES[i]:
            out.append(local(src.at[pl.ds(part * half[i] + row, rows), :], dst.at[:, pl.ds(col, cols)], keep_sem.at[1, i]))
        return out

    def last_copies(i, axis):
        src, dst = held[i].at[LAST, axis], last.at[i, axis]
        return [
            local(src.at[pl.ds(part * half[i] + row, rows), :], dst.at[part, :, pl.ds(col, cols)], keep_sem.at[2, i])
            for part in range(2)
            for row, col, rows, cols in PIECES[i]
        ]

    def block_to_core(i, t, axis):
        dst = block(i, t, by_x if axis == 0 else by_y)
        return remote(held[i].at[t, axis], dst, send_sem.at[4, i], gather_sem.at[1, i], to_core)

    def in_copies(i, t):
        layer, sub = where(t)
        rows = pl.ds(pl.multiple_of(sub * size[i], size[i]), size[i])
        mine = pl.ds(pl.multiple_of(me * ROWS[i] + sub * size[i], size[i]), size[i])
        return [
            local(w[i].at[layer, mine, :], w_in[i], in_sem.at[0, i]),
            local(m[i].at[layer, rows, :], m_in[i], in_sem.at[1, i]),
            local(v[i].at[layer, rows, :], v_in[i], in_sem.at[2, i]),
        ]

    def mv_copies(i, t):
        layer, sub = where(t)
        rows = pl.ds(pl.multiple_of(sub * size[i], size[i]), size[i])
        return [
            local(m_new[i], m_out[i].at[layer, rows, :], mv_sem.at[0, i]),
            local(v_new[i], v_out[i].at[layer, rows, :], mv_sem.at[1, i]),
        ]

    def start_core(t, order=((0, 1), (2, 3)), weights=(0, 1, 2)):
        for pieces in order:
            for i in weights:
                for piece in pieces:
                    core_copy(i, t, piece).start()

    def start_own(t):
        for i in range(3):
            own_copy(i, t).start()

    def reduce_first(t):
        slot = lax.rem(t, RING)
        for i in range(3):
            own_copy(i, t).wait()
            for axis in range(2):
                core_copy(i, t, axis).wait_recv()
                for a in range(2):
                    bx, by = (1 - x, a) if axis == 0 else (a, 1 - y)

                    def add(row, col, i=i, bx=bx, by=by, axis=axis):
                        at = (pl.ds(axis * half[i] + row, WIDE[0]), pl.ds(col, WIDE[1]))
                        mine = own[i][(slot, bx, by, *at)].astype(F32)
                        core[i][(t, bx, by, *at)] = (mine + core[i][(t, bx, by, *at)].astype(F32)).astype(BF16)

                    tiles(half[i], COLS[i], add, WIDE)
                first_copy(i, t, axis).start()

    def reduce_second(t):
        slot = lax.rem(t, RING)
        for i in range(3):
            for axis in range(2):
                core_copy(i, t, axis + 2).wait_recv()
                first_copy(i, t, axis).wait_recv()
                bx, by = (x, 1 - y) if axis == 0 else (1 - x, y)
                came = 1 - y if axis == 0 else 1 - x

                def add(row, col, i=i, bx=bx, by=by, axis=axis, came=came):
                    at = (pl.ds(axis * half[i] + row, WIDE[0]), pl.ds(col, WIDE[1]))
                    mine = own[i][(slot, bx, by, *at)].astype(F32) + core[i][(t, bx, by, *at)].astype(F32)
                    other = first[i][t, axis, came, pl.ds(row, WIDE[0]), pl.ds(col, WIDE[1])].astype(F32)
                    core[i][(t, bx, by, *at)] = (mine + other).astype(BF16)

                tiles(half[i], COLS[i], add, WIDE)
                second_copy(i, t, axis).start()

    def update(t):
        slot = lax.rem(t, RING)
        for i in range(3):
            for copy in in_copies(i, t):
                copy.wait()

            @pl.when(t > 0)
            def _(i=i):
                for copy in mv_copies(i, t - 1):
                    copy.wait()

            for axis in range(2):
                second_copy(i, t, axis).wait_recv()
                came = y if axis == 0 else x

                def adamw(row, col, i=i, axis=axis, came=came):
                    at = (pl.ds(axis * half[i] + row, TILE[0]), pl.ds(col, TILE[1]))
                    there = (pl.ds(row, TILE[0]), pl.ds(col, TILE[1]))
                    total = own[i][(slot, x, y, *at)].astype(F32) + core[i][(t, x, y, *at)].astype(F32)
                    total = total + first[i][(t, axis, came, *there)].astype(F32) + second[i][(t, axis, *there)].astype(F32)
                    grad = total.astype(BF16).astype(F32)
                    weight = w_in[i][at].astype(F32)
                    mm = 0.9 * m_in[i][at] + 0.1 * grad
                    vv = 0.95 * v_in[i][at] + 0.05 * grad * grad
                    step = mm * lax.rsqrt(vv + 1e-8) + 0.1 * weight
                    m_new[i][at] = mm
                    v_new[i][at] = vv
                    fresh[i][(t, *at)] = (weight - 0.02 * step).astype(BF16)

                tiles(half[i], COLS[i], adamw)
            for copy in block_copies(i, t) + mv_copies(i, t):
                copy.start()

            @pl.when(t + 1 < CHUNKS)
            def _(i=i):
                for copy in in_copies(i, t + 1):
                    copy.start()

    def forward(t):
        for group, start in enumerate(STARTS):

            @pl.when(jnp.logical_and(t >= start, t < start + GROUPS[group]))
            def _(group=group):
                for i in range(3):
                    for axis in range(2):
                        block_copies(i, t)[axis].wait_recv()
                        for copy in keep_copies(i, t, axis, group):
                            copy.start()

                        @pl.when(t < LAST)
                        def _(i=i, axis=axis):
                            block_to_core(i, t, axis).start()

                        @pl.when(t == LAST)
                        def _(i=i, axis=axis):
                            for copy in last_copies(i, axis):
                                copy.start()

    start_own(0)

    @pl.when(c == 0)
    def _():
        start_core(0)
        start_core(1)

    @pl.when(c == 1)
    def _():
        start_core(1)
        start_core(0, ((2, 3), (0, 1)), (2, 1, 0))

    for i in range(3):
        for copy in in_copies(i, 0):
            copy.start()

    def step(k, carry):
        @pl.when(k < CHUNKS - 2)
        def _():
            start_core(k + 2)

        @pl.when(k < CHUNKS - 1)
        def _():
            start_own(k + 1)

        for lag, stage in enumerate((reduce_first, reduce_second, update, forward)):

            @pl.when(jnp.logical_and(k >= lag, k < CHUNKS + lag))
            def _(lag=lag, stage=stage):
                stage(k - lag)

        return carry

    lax.fori_loop(0, CHUNKS + 3, step, 0)

    for i in range(3):
        for copy in mv_copies(i, LAST):
            copy.wait()
        part = w_out[i].at[:, pl.ds(0, 4 * ROWS[i]), :]
        most = held[i].at[pl.ds(0, LAST)]
        local(fresh[i], fresh[i], gather_sem.at[0, i]).wait()
        local(most, most, gather_sem.at[1, i]).wait()
        for kind, ref in ((0, core[i]), (1, first[i]), (2, second[i]), (3, part), (4, most)):
            local(ref, ref, send_sem.at[kind, i]).wait()
        for kind, ref in ((0, held[i]), (1, fresh[i]), (2, held[i].at[0])):
            local(ref, ref, keep_sem.at[kind, i]).wait()


PIECES = (((0, 0, 16, 3072),), ((0, 0, 16, 3072),), tuple((16 * p, 1024 * p, 16, 1024) for p in range(3)))


def write_weights(me_ref, *refs):
    w, w_out, ring, sem = refs[:3], refs[3:6], refs[6:9], refs[9]
    me = me_ref[0]
    x, y = lax.div(me, 4), lax.rem(lax.div(me, 2), 2)
    size = [r // HALVES for r in ROWS]
    jobs = 3 * LAYERS * HALVES

    def copies(i, k):
        t, r = lax.div(k, 3), lax.rem(k, 3)
        bx = jnp.where(r == 1, 1 - x, x)
        by = jnp.where(r == 2, 1 - y, y)
        rows = pl.ds(pl.multiple_of(lax.rem(t, HALVES) * size[i], size[i]), size[i])
        at = (lax.div(t, HALVES), bx, by, slice(None), rows, slice(None))
        slot = lax.rem(k, DEEP)
        buf = ring[i].at[slot]
        return pltpu.make_async_copy(w[i].at[at], buf, sem.at[0, slot, i]), pltpu.make_async_copy(buf, w_out[i].at[at], sem.at[1, slot, i])

    ahead = DEEP // 2
    for k in range(ahead):
        for i in range(3):
            copies(i, jnp.int32(k))[0].start()

    def step(k, carry):
        for i in range(3):
            into, out = copies(i, k)
            into.wait()
            out.start()

            @pl.when(k >= ahead)
            def _(i=i):
                copies(i, k - ahead)[1].wait()

            @pl.when(k + ahead < jobs)
            def _(i=i):
                copies(i, k + ahead)[0].start()

        return carry

    lax.fori_loop(0, jobs, step, 0)
    for k in range(jobs - ahead, jobs):
        for i in range(3):
            copies(i, jnp.int32(k))[1].wait()


DEEP = 8
HALVES = 2


def write_moments(*refs):
    src, dst, buf, sem = refs[:6], refs[6:12], refs[12:18], refs[18]

    def copies(i, n):
        at = (n // 2, pl.ds(n % 2 * (src[i].shape[1] // 2), src[i].shape[1] // 2))
        return pltpu.make_async_copy(src[i].at[at], buf[i].at[at], sem.at[0, i, n]), pltpu.make_async_copy(buf[i].at[at], dst[i].at[at], sem.at[1, i, n])

    every = [(i, n) for i in range(6) for n in range(4)]
    for job in every:
        copies(*job)[0].start()
    for job in every:
        copies(*job)[0].wait()
        copies(*job)[1].start()
    for job in every:
        copies(*job)[1].wait()


def write_diag(groups, me_ref, *refs):
    arrays, refs = refs[: 4 * len(groups) + (0 in groups)], refs[4 * len(groups) + (0 in groups) :]
    w_out, sem = refs[3:6], refs[6]
    me = me_ref[0]
    x, y, c = lax.div(me, 4), lax.rem(lax.div(me, 2), 2), lax.rem(me, 2)

    def write(i, t, part, owner, src):
        size = ROWS[i] // SUBS
        start = owner * ROWS[i] + lax.rem(t, SUBS) * size + part * (size // 2)
        for row, col, rows, cols in PIECES[i]:
            dst = w_out[i].at[lax.div(t, SUBS), pl.ds(pl.multiple_of(start + row, 16), rows), :]
            pltpu.make_async_copy(src.at[:, pl.ds(col, cols)], dst, sem).start()

    for n, group in enumerate(groups):
        mine_a, mine_b, other_a, other_b = arrays[4 * n : 4 * n + 4]

        def each(j, carry, group=group, sources=((0, c, mine_a), (1, c, mine_b), (0, 1 - c, other_a), (1, 1 - c, other_b))):
            diag = 6 - 4 * x - 2 * y
            for i in range(3):
                for part, owner, src in sources:
                    write(i, j + STARTS[group], part, diag + owner, src.at[i, j])
            return carry

        lax.fori_loop(0, GROUPS[group], each, 0)
    if 0 in groups:
        last = arrays[-1]
        for i in range(3):
            for axis, owner in ((0, 4 * (1 - x) + 2 * y + 1 - c), (1, 4 * x + 2 * (1 - y) + 1 - c)):
                for part in range(2):
                    write(i, jnp.int32(LAST), part, owner, last.at[i, axis, part])
    for src in arrays:
        pltpu.make_async_copy(src, src, sem).wait()


def scratch(lead, dtype=BF16, lane=lambda i: ROWS[i] // SUBS):
    return [pltpu.VMEM((*lead, lane(i), COLS[i]), dtype) for i in range(3)]


def step(*arrays):
    g, w, m, v = (arrays[i : i + 3] for i in (0, 3, 6, 9))
    g = [t.reshape(LAYERS, 2, 2, 2, ROWS[i], COLS[i]) for i, t in enumerate(g)]
    halves = lambda i: ROWS[i] // SUBS // 2
    dma = pltpu.SemaphoreType.DMA
    hbm = pl.BlockSpec(memory_space=pltpu.HBM)
    like = [jax.ShapeDtypeStruct(t.shape, t.dtype) for t in (*w, *m, *v)]
    out = pl.pallas_call(
        kernel,
        out_shape=like + [jax.ShapeDtypeStruct((3, n, 16, 3072), BF16) for n in GROUPS for _ in range(2)] + [jax.ShapeDtypeStruct((3, 2, 2, 16, 3072), BF16)],
        in_specs=[hbm] * 12,
        out_specs=[hbm] * (10 + 2 * len(GROUPS)),
        scratch_shapes=[
            *scratch((CHUNKS, 2, 2)),
            *scratch((CHUNKS, 2, 2), lane=halves),
            *scratch((CHUNKS, 2), lane=halves),
            *scratch((RING, 2, 2)),
            *scratch((CHUNKS, 2)),
            *scratch((CHUNKS,)),
            *scratch(()),
            *scratch((), F32),
            *scratch((), F32),
            *scratch((), F32),
            *scratch((), F32),
            dma((CHUNKS, 4, 3)),
            dma((RING, 3)),
            dma((CHUNKS, 2, 3)),
            dma((CHUNKS, 2, 3)),
            dma((CHUNKS, 2, 3)),
            dma((3, 3)),
            dma((2, 3)),
            dma((5, 3)),
            dma((2, 3)),
            dma((3, 3)),
        ],
        compiler_params=pltpu.CompilerParams(collective_id=0, has_side_effects=True, vmem_limit_bytes=62 * 2**20),
        name="step",
    )(*g, *w, *m, *v)
    gathered, moments, pass_on, last = out[:3], out[3:9], [out[9 + 2 * n : 11 + 2 * n] for n in range(len(GROUPS))], out[-1]

    def swap(t, far):
        return lax.ppermute(t, "dp", [(i, i ^ far) for i in range(8)])

    mine = [[swap(pair[0], 4), swap(pair[1], 2)] for pair in pass_on]
    other = [[swap(t, 1) for t in pair] for pair in mine]
    last = swap(last, 1)

    me = lax.axis_index("dp").astype(jnp.int32).reshape(1)
    smem, vmem = pl.BlockSpec(memory_space=pltpu.SMEM), pl.BlockSpec(memory_space=pltpu.VMEM)

    def writer(body, operands, in_specs, outs, scratch_shapes, limit, flops, aliases={}):
        return pl.pallas_call(
            body,
            out_shape=outs,
            in_specs=in_specs,
            out_specs=[hbm] * len(outs),
            scratch_shapes=scratch_shapes,
            input_output_aliases=aliases,
            compiler_params=pltpu.CompilerParams(vmem_limit_bytes=limit * 2**20),
            cost_estimate=pl.CostEstimate(flops=flops, bytes_accessed=flops // 40, transcendentals=0),
        )(*operands)

    blocks = [t.reshape(LAYERS, 2, 2, 2, ROWS[i], COLS[i]) for i, t in enumerate(gathered)]
    shapes = [jax.ShapeDtypeStruct(t.shape, t.dtype) for t in blocks]
    ring = [*(pltpu.VMEM((DEEP, 2, ROWS[i] // HALVES, COLS[i]), BF16) for i in range(3)), dma((2, DEEP, 3))]
    whole = writer(write_weights, (me, *blocks), [smem] + [hbm] * 3, shapes, ring, 57, 2_000_000_000)
    buffers = [*(pltpu.VMEM(t.shape, F32) for t in moments), dma((2, 6, 4))]
    moments = writer(write_moments, moments, [hbm] * 6, like[3:], buffers, 55, 1_400_000_000)
    whole = [t.reshape(w[i].shape) for i, t in enumerate(whole)]
    for groups in WRITES:
        late = [t for n in groups for t in (*mine[n], *other[n])] + [last] * (0 in groups)
        at = 1 + len(late)
        specs = [smem] + [vmem] * len(late) + [hbm] * 3
        body = functools.partial(write_diag, groups)
        whole = writer(body, (me, *late, *whole), specs, like[:3], [dma], 12, 100_000_000, {at + i: i for i in range(3)})
    return (*whole, *moments)


def solution(mesh):
    all_of, cut = P(None, None, None), P(None, "dp", None)
    return jax.shard_map(
        step,
        mesh=mesh,
        in_specs=(P(("rep", "dp"), None, None, None),) * 3 + (all_of,) * 3 + (cut,) * 6,
        out_specs=(P("rep", None, None),) * 3 + (P("rep", "dp", None),) * 6,
        check_vma=False,
    )
```
